256 devices in a mesh: dom: 32 (over y, x, z_hi), orb: 8 (over z_lo, core).
Axes of the slice: x: 4, y: 4, z: 8 (z_hi: 2, z_lo: 4; z = z_hi * 4 + z_lo), core: 2. Of those that a mesh axis runs over, the one named last changes fastest.
Arguments:
- orbitals: float32 [16, 256, 64, 128], P('orb', 'dom'), may hold values from -10.8 to 10.8
- initial_guess: float32 [16, 256, 64, 128], P('orb', 'dom'), may hold values from -350 to 350
- potential: float32 [256, 64, 128], P('dom'), may hold values from 0.1 to 2
- perturbation: float32 [256, 64, 128], P('dom'), may hold values from -6 to 6
- level_shifts: float32 [16], replicated, may hold values from 0.05 to 2
- assignment: int32 [16], P('orb'), may hold values from 0 to 15, each once
Outputs:
- updated_response: float32 [16, 256, 64, 128], P('orb', 'dom')
The draws below stay inside these ranges and needn't reach their ends.
Inputs may be any that keep to these rules, and one draw needn't show every extreme that they name: `assignment`: every energy index appears in exactly one slot.
All inputs are finite; a program needn't handle non-finite values.
Results may differ from the reference program's by a relative error of at most 0.0003.
Values sent between devices are 32-bit elements; how exact they have to be, the bound alone decides.
A program may use at most 128 MiB of HBM per device.

```python
import math
import jax
import jax.numpy as jnp
from jax import lax

NY = 64
NZ = 128
SWEEPS = 2
COARSE = 4
NX = 256
ORBITALS = 16


def orbital_values(key):
    extent = (ORBITALS, NX, NY, NZ)
    sample = jnp.clip(jax.random.normal(jax.random.fold_in(key, 101), extent, jnp.float32), -6.0, 6.0)
    envelope = 0.6 + 1.2 * jnp.arange(NX, dtype=jnp.float32) / NX
    return sample * envelope[None, :, None, None]


def draw_orbitals(key, part):
    return orbital_values(key)


def draw_initial_guess(key, part):
    orbit_values = orbital_values(key)
    extent = (ORBITALS, NX, NY, NZ)
    coupling = 0.5 * jnp.clip(jax.random.normal(jax.random.fold_in(key, 202), (ORBITALS, ORBITALS), jnp.float32), -4.0, 4.0)
    jitter = jnp.clip(jax.random.normal(jax.random.fold_in(key, 303), extent, jnp.float32), -6.0, 6.0)
    blended = jnp.einsum('ji,jxyz->ixyz', coupling, orbit_values)
    return blended + 0.5 * jitter


def level_of(key, shape, shards, smallest, high):
    def one(position, parts):
        heights = jax.random.uniform(jax.random.fold_in(jax.random.fold_in(key, 6), position), (parts,), jnp.float32, smallest / len(shards), high / len(shards))
        return jnp.repeat(jnp.exp(heights), shape[position] // parts).reshape((-1,) + (1,) * (len(shape) - position - 1))

    gain = one(*shards[0])
    for cut in shards[1:]:
        gain = gain * one(*cut)
    return gain


def normal_values(stream_key, dims, spread, most, split=(), kind=jnp.bfloat16):
    drawn = spread * jax.random.normal(stream_key, dims, jnp.float32)
    if split:
        drawn = drawn * level_of(stream_key, dims, split, -0.22, 0.18)
    return jnp.clip(drawn, -most, most).astype(kind)


def setup_inputs(seed: int = 0) -> dict:
    seeds = jax.random.split(jax.random.key(seed), 7)
    return {
        "orbitals": draw_orbitals(jax.random.fold_in(seeds[6], 71), 0),
        "initial_guess": draw_initial_guess(jax.random.fold_in(seeds[6], 71), 0),
        "potential": jnp.clip(0.1 + 1.9 * jax.random.uniform(seeds[2], (NX, NY, NZ), jnp.float32) ** level_of(seeds[2], (NX, NY, NZ), ((0, 32),), -0.2, 0.2), 0.1, 2.0),
        "perturbation": normal_values(seeds[3], (NX, NY, NZ), 1.0, 6.0, ((0, 32),), jnp.float32),
        "level_shifts": jnp.clip(jnp.exp(jax.random.uniform(seeds[4], (ORBITALS,), jnp.float32, math.log(0.05), math.log(2.0))), 0.05, 2.0),
        "assignment": jax.random.permutation(seeds[5], ORBITALS).astype(jnp.int32),
    }


OMEGA = 0.8
KINETIC = 8.0


def apply_level(field_values, potential_level, shift_value, level):
    inverse_area = 0.25 ** level
    neighbours = (jnp.roll(field_values, -1, 0) + jnp.roll(field_values, 1, 0)) + (jnp.roll(field_values, -1, 1) + jnp.roll(field_values, 1, 1)) + (jnp.roll(field_values, -1, 2) + jnp.roll(field_values, 1, 2))
    return KINETIC * inverse_area * (6.0 * field_values - neighbours) + (potential_level + shift_value) * field_values


def diagonal_of(potential_level, shift_value, level):
    return 6.0 * KINETIC * 0.25 ** level + potential_level + shift_value


def relax(estimate, source, potential_level, shift_value, level):
    applied = apply_level(estimate, potential_level, shift_value, level)
    return estimate + OMEGA * (source - applied) / diagonal_of(potential_level, shift_value, level)


def coarsen(field_values):
    sx, sy, sz = field_values.shape
    return field_values.reshape(sx // 2, 2, sy // 2, 2, sz // 2, 2).mean(axis=(1, 3, 5))


def refine(field_values):
    return jnp.repeat(jnp.repeat(jnp.repeat(field_values, 2, 0), 2, 1), 2, 2)


def reference(orbitals, initial_guess, potential, perturbation, level_shifts, assignment):
    shifts = level_shifts[assignment.astype(jnp.int32)]
    levels = [potential]
    levels.append(coarsen(levels[0]))
    levels.append(coarsen(levels[1]))

    def solve_one(inputs):
        orbital, guess, shift_value = inputs
        source = -(perturbation * orbital)
        sources = [source - apply_level(guess, levels[0], shift_value, 0)]
        estimates = []
        for level in range(2):
            current = sources[level]
            estimate = OMEGA * current / diagonal_of(levels[level], shift_value, level)
            for sweep_index in range(SWEEPS - 1):
                estimate = relax(estimate, current, levels[level], shift_value, level)
            remainder = current - apply_level(estimate, levels[level], shift_value, level)
            estimates.append(estimate)
            sources.append(coarsen(remainder))
        lower = OMEGA * sources[2] / diagonal_of(levels[2], shift_value, 2)
        for sweep_index in range(COARSE - 1):
            lower = relax(lower, sources[2], levels[2], shift_value, 2)
        for level in (1, 0):
            estimate = estimates[level] + refine(lower)
            for sweep_index in range(SWEEPS):
                estimate = relax(estimate, sources[level], levels[level], shift_value, level)
            lower = estimate
        return guess + lower

    update = lax.map(solve_one, (orbitals, initial_guess, shifts))
    flat_orbit = orbitals.reshape(ORBITALS, -1)
    flat_update = update.reshape(ORBITALS, -1)
    intersection = jnp.einsum("jc,ic->ji", flat_orbit, flat_update, precision=lax.Precision.HIGHEST) / (NX * NY * NZ)
    result = flat_update - jnp.einsum("ji,jc->ic", intersection, flat_orbit, precision=lax.Precision.HIGHEST)
    return result.reshape(update.shape)
```

```python
import functools

import jax
import jax.numpy as jnp
from jax import lax
from jax.experimental import pallas as pl
from jax.experimental.pallas import tpu as pltpu
from jax.sharding import PartitionSpec as P

OMEGA = 0.8
KINETIC = 8.0
MESH = pl.DeviceIdType.MESH
F32 = jnp.float32


def turn(x, shift, axis):
    return pltpu.roll(x, shift % x.shape[axis], axis)


def ring(x, step):
    ya, za = x.ndim - 2, x.ndim - 1
    return (turn(x, 1, ya) + turn(x, -1, ya)) + (turn(x, step, za) + turn(x, -step, za))


def lane_bit(shape, bit):
    return (lax.broadcasted_iota(jnp.int32, shape, len(shape) - 1) & bit) == 0


def pair(first, second, bit):
    za = first.ndim - 1
    return jnp.where(
        lane_bit(first.shape, bit), first + turn(first, -bit, za), second + turn(second, bit, za)
    )


def split(packed, bit):
    za = packed.ndim - 1
    clear = lane_bit(packed.shape, bit)
    return (
        jnp.where(clear, packed, turn(packed, bit, za)),
        jnp.where(clear, turn(packed, -bit, za), packed),
    )


def kernel(
    cells, orb_in, guess_in, pot_in, pert_in, table, slot, out,
    orbs, g, pot, pert, gh, st_out, st_in, c2_out, c2_in, fe_out, fe_in,
    f, w, ea, eb, f1, c1, w1, e1, f2_out, f2_in, rows, gram, part1, part2, coef,
    load_sem, halo_send, halo_recv, wide_send, wide_recv, ag_send, ag_recv,
    gram_send, gram_recv, sum_send, sum_recv,
):
    d = lax.axis_index("dom")
    o = lax.axis_index("orb")
    doms = lax.axis_size("dom")
    layers, half, quarter = 8, 4, 2

    loads = [
        pltpu.make_async_copy(guess_in, g.at[:, pl.ds(1, layers)], load_sem.at[0]),
        pltpu.make_async_copy(orb_in, orbs.at[o], load_sem.at[1]),
        pltpu.make_async_copy(pot_in, pot, load_sem.at[2]),
        pltpu.make_async_copy(pert_in, pert, load_sem.at[3]),
    ]
    for copy in loads:
        copy.start()

    barrier = pltpu.get_barrier_semaphore()
    plane = lax.div(d, 8) * 8
    near = [lax.rem(d + doms + k, doms) for k in (-3, -2, -1, 1, 2, 3)]
    line = [plane + lax.rem(d - plane + k, 8) for k in range(1, 8)]
    far = [lax.rem(d + 8 * k, doms) for k in range(1, 4)]
    chip = lax.div(o, 2)
    mate = o + 1 - 2 * lax.rem(o, 2)
    others = [mate] + [lax.rem(o + 2 * k, 8) for k in range(1, 4)]
    for there in near + line + far:
        pl.semaphore_signal(barrier, inc=1, device_id={"dom": there}, device_id_type=MESH)
    for there in others:
        pl.semaphore_signal(barrier, inc=1, device_id={"orb": there}, device_id_type=MESH)

    shift = [table[slot[i]] for i in range(2)]
    base = [6.0 * KINETIC + s for s in shift]
    zero = jnp.zeros((64, 128), F32)
    for i in range(2):
        g[i, 0] = zero
        g[i, layers + 1] = zero
    for copy in loads:
        copy.wait()

    def start_layer(l, carry):
        p, q = pot[l], pert[l]
        for i in range(2):
            x = g[i, l + 1]
            diag = p + base[i]
            around = ring(x, 1) + (g[i, l] + g[i, l + 2])
            f[i, l + 1] = KINETIC * around - diag * x - q * orbs[o, i, l]
            w[i, l + 1] = OMEGA / diag
        return carry

    lax.fori_loop(0, layers, start_layer, 0)
    for side, (edge, inner) in enumerate(((1, 2), (layers, layers - 1))):
        for i in range(2):
            fe_out[side, 0, i] = f[i, edge]
            fe_out[side, 1, i] = w[i, inner] * f[i, inner]

    for q in range(half):
        t = pot[2 * q] + pot[2 * q + 1]
        rows[q] = pair(t, t, 1)
    for q in range(half):
        c1[q + 2] = 0.125 * (rows[q, pl.ds(0, 32, stride=2)] + rows[q, pl.ds(1, 32, stride=2)])
    even = lane_bit((32, 128), 1)
    st_out[0, pl.ds(0, 64)] = pot[0]
    st_out[1, pl.ds(0, 64)] = pot[layers - 1]
    st_out[0, pl.ds(64, 32)] = jnp.where(even, c1[2], c1[3])
    st_out[1, pl.ds(64, 32)] = jnp.where(even, c1[4], c1[5])
    for q in range(quarter):
        t = c1[2 * q + 2] + c1[2 * q + 3]
        rows[q, pl.ds(0, 32)] = pair(t, t, 2)
    c2 = [
        0.125 * (rows[q, pl.ds(0, 16, stride=2)] + rows[q, pl.ds(1, 16, stride=2)])
        for q in range(quarter)
    ]
    low = lane_bit((16, 128), 2)
    c2_out[...] = jnp.where(low, c2[0], c2[1])

    pl.semaphore_wait(barrier, len(near) + len(line) + len(far) + len(others))

    def to_dom(src, dst, sends, recvs, k, there):
        return pltpu.make_async_remote_copy(
            src_ref=src, dst_ref=dst, send_sem=sends.at[k], recv_sem=recvs.at[k],
            device_id={"dom": there}, device_id_type=MESH,
        )

    below, above = near[2], near[3]
    first = []
    for side, there in ((0, below), (1, above)):
        edge = 1 if side == 0 else layers
        first += [
            to_dom(fe_out.at[side], fe_in.at[1 - side], halo_send, halo_recv, side, there),
            to_dom(g.at[:, edge], gh.at[1 - side], halo_send, halo_recv, 2 + side, there),
            to_dom(st_out.at[side], st_in.at[1 - side], halo_send, halo_recv, 4 + side, there),
        ]
    for copy in first:
        copy.start()
    coarse = [to_dom(c2_out, c2_in.at[5 - k], wide_send, wide_recv, k, near[k]) for k in range(6)]
    for copy in coarse:
        copy.start()

    def hand(block, k, there):
        return pltpu.make_async_remote_copy(
            src_ref=orbs.at[block], dst_ref=orbs.at[block],
            send_sem=ag_send.at[k], recv_sem=ag_recv.at[k],
            device_id={"orb": there}, device_id_type=MESH,
        )

    def up(n):
        return hand(o - 2 * n, n, o + 2)

    def down(n):
        return hand(o + 2 * n, 3 + n, o - 2)

    def over_up(n):
        return hand(o - 2 * n, 6 + n, mate)

    def over_down(n):
        return hand(o + 2 * n, 9 + n, mate)

    across = hand(o, 6, mate)

    def open_gather():
        across.start()

        @pl.when(chip < 3)
        def _():
            up(0).start()

        @pl.when(chip > 0)
        def _():
            down(0).start()

    def relay(n):
        @pl.when(chip >= n)
        def _():
            hand(o - 2 * n, n - 1, o + 2).wait_recv()
            over_up(n).start()

        if n < 3:

            @pl.when((chip >= n) & (chip < 3))
            def _():
                up(n).start()

        @pl.when(chip <= 3 - n)
        def _():
            hand(o + 2 * n, 3 + n - 1, o - 2).wait_recv()
            over_down(n).start()

        if n < 3:

            @pl.when((chip <= 3 - n) & (chip > 0))
            def _():
                down(n).start()

    open_gather()

    for copy in first:
        copy.wait_recv()

    for i in range(2):
        f[i, 1] = f[i, 1] + KINETIC * gh[0, i]
        f[i, layers] = f[i, layers] + KINETIC * gh[1, i]
        for side, (beyond, edge, rim) in enumerate(((0, 1, 0), (layers + 1, layers, 11))):
            f[i, beyond] = fe_in[side, 0, i] + KINETIC * g[i, edge]
            w[i, beyond] = OMEGA / (st_in[side, pl.ds(0, 64)] + base[i])
            ea[i, rim] = fe_in[side, 1, i]
    c1[0], c1[1] = split(st_in[0, pl.ds(64, 32)], 1)
    c1[6], c1[7] = split(st_in[1, pl.ds(64, 32)], 1)

    def begin(l, carry):
        for i in range(2):
            ea[i, l + 1] = w[i, l] * f[i, l]
        return carry

    lax.fori_loop(0, layers + 2, begin, 0)

    def sweep_down(l, carry):
        for i in range(2):
            around = ring(ea[i, l + 1], 1) + (ea[i, l] + ea[i, l + 2])
            eb[i, l + 1] = w[i, l] * ((2.0 - OMEGA) * f[i, l] + KINETIC * around)
        return carry

    lax.fori_loop(0, layers + 2, sweep_down, 0)
    second = [
        to_dom(eb.at[:, 3], eb.at[:, 11], halo_send, halo_recv, 6, below),
        to_dom(eb.at[:, 8], eb.at[:, 0], halo_send, halo_recv, 7, above),
    ]

    def remainder(q, carry):
        total = []
        for i in range(2):
            parts = []
            for h in range(2):
                l = 2 * q + h
                x = eb[i, l + 2]
                around = ring(x, 1) + (eb[i, l + 1] + eb[i, l + 3])
                parts.append(f[i, l + 1] + KINETIC * around - (pot[l] + base[i]) * x)
            total.append(parts[0] + parts[1])
        rows[q] = pair(total[0], total[1], 1)
        return carry

    lax.fori_loop(0, half, remainder, 0)
    for q in range(half):
        f1[q + 2] = 0.125 * (rows[q, pl.ds(0, 32, stride=2)] + rows[q, pl.ds(1, 32, stride=2)])
    third = [
        to_dom(f1.at[pl.ds(2, 2)], f1.at[pl.ds(6, 2)], halo_send, halo_recv, 8, below),
        to_dom(f1.at[pl.ds(4, 2)], f1.at[pl.ds(0, 2)], halo_send, halo_recv, 9, above),
    ]
    for copy in third + second:
        copy.start()
    relay(1)

    k1, k2 = KINETIC / 4, KINETIC / 16
    both = jnp.where(even, shift[0], shift[1])
    for q in range(8):
        w1[q] = OMEGA / (c1[q] + (6.0 * k1 + both))
    for copy in coarse:
        copy.wait_recv()
    both2 = jnp.where(lane_bit((16, 128), 1), shift[0], shift[1])
    c2s = []
    for k in range(3):
        c2s += split(c2_in[k], 2)
    c2s += c2
    for k in range(3, 6):
        c2s += split(c2_in[k], 2)
    w2 = jnp.stack([OMEGA / (c + (6.0 * k2 + both2)) for c in c2s[1:13]])

    for copy in third:
        copy.wait_recv()
    fs, ws = f1[...], w1[...]
    e = ws * fs
    e = ws[1:7] * ((2.0 - OMEGA) * fs[1:7] + k1 * (ring(e[1:7], 2) + (e[:6] + e[2:])))
    e1[pl.ds(2, 6)] = e
    x = e[1:5]
    r = fs[2:6] + k1 * (ring(x, 2) + (e[:4] + e[2:])) - (c1[pl.ds(2, 4)] + (6.0 * k1 + both)) * x
    for q in range(quarter):
        t = r[2 * q] + r[2 * q + 1]
        rows[q, pl.ds(0, 32)] = pair(t, t, 2)
    f2 = [
        0.125 * (rows[q, pl.ds(0, 16, stride=2)] + rows[q, pl.ds(1, 16, stride=2)])
        for q in range(quarter)
    ]
    f2_out[...] = jnp.where(low, f2[0], f2[1])
    fourth = [
        to_dom(f2_out, f2_in.at[5 - k], wide_send, wide_recv, 6 + k, near[k]) for k in range(6)
    ]
    fifth = [
        to_dom(e1.at[pl.ds(4, 2)], e1.at[pl.ds(8, 2)], halo_send, halo_recv, 10, below),
        to_dom(e1.at[pl.ds(4, 2)], e1.at[pl.ds(0, 2)], halo_send, halo_recv, 11, above),
    ]
    for copy in fourth + fifth:
        copy.start()
    relay(2)
    for copy in fourth:
        copy.wait_recv()

    f2s = []
    for k in range(3):
        f2s += split(f2_in[k], 2)
    f2s += f2
    for k in range(3, 6):
        f2s += split(f2_in[k], 2)
    f2v = jnp.stack(f2s[1:13])
    e = w2 * f2v
    for n in range(1, 4):
        inner = slice(n, 12 - n)
        x = e[1:-1]
        e = (1.0 - OMEGA) * x + w2[inner] * (f2v[inner] + k2 * (ring(x, 4) + (e[:-2] + e[2:])))

    for q in range(6):
        rows[q, pl.ds(0, 16, stride=2)] = e[q]
        rows[q, pl.ds(1, 16, stride=2)] = e[q]
    for copy in fifth:
        copy.wait_recv()
    e = jnp.stack([e1[l + 3] + rows[l // 2 + 2, pl.ds(0, 32)] for l in range(-3, 7)])
    for n in range(2):
        inner = slice(n, 8 - n)
        x = e[1:-1]
        e = (1.0 - OMEGA) * x + ws[inner] * (fs[inner] + k1 * (ring(x, 2) + (e[:-2] + e[2:])))
    for q in range(6):
        rows[q, pl.ds(0, 32, stride=2)] = e[q]
        rows[q, pl.ds(1, 32, stride=2)] = e[q]

    for copy in second:
        copy.wait_recv()

    def correct(q, carry):
        fields = split(rows[q], 1)
        for i in range(2):
            for h in range(2):
                ea[i, 2 * q + h] = eb[i, 2 * q + h] + fields[i]
        return carry

    lax.fori_loop(0, 6, correct, 0)
    for copy in second:
        copy.wait_send()

    def sweep_up(l, carry):
        for i in range(2):
            x = ea[i, l + 1]
            around = ring(x, 1) + (ea[i, l] + ea[i, l + 2])
            eb[i, l + 1] = (1.0 - OMEGA) * x + w[i, l] * (f[i, l] + KINETIC * around)
        return carry

    lax.fori_loop(0, layers + 2, sweep_up, 0)

    def sweep_last(l, carry):
        for i in range(2):
            x = eb[i, l + 2]
            around = ring(x, 1) + (eb[i, l + 1] + eb[i, l + 3])
            ea[i, l] = g[i, l + 1] + (
                (1.0 - OMEGA) * x + w[i, l + 1] * (f[i, l + 1] + KINETIC * around)
            )
        return carry

    lax.fori_loop(0, layers, sweep_last, 0)

    relay(3)
    across.wait_recv()
    for n in range(1, 4):

        @pl.when(chip >= n)
        def _():
            over_up(n).wait_recv()

        @pl.when(chip <= 3 - n)
        def _():
            over_down(n).wait_recv()

    def products(n, sums):
        l, r = lax.div(n, 8), pl.ds(pl.multiple_of(lax.rem(n, 8) * 8, 8), 8)
        u = [ea[i, l, r, :] for i in range(2)]
        new = []
        for j in range(16):
            x = orbs[j // 2, j % 2, l, r, :]
            new += [sums[2 * j + i] + x * u[i] for i in range(2)]
        return tuple(new)

    sums = lax.fori_loop(0, 64, products, (jnp.zeros((8, 128), F32),) * 32)
    for m in range(32):
        gram[pl.ds(m, 1), :] = jnp.sum(sums[m], axis=0, keepdims=True)
    diagonal = lax.broadcasted_iota(jnp.int32, (32, 128), 0) == lax.broadcasted_iota(
        jnp.int32, (32, 128), 1
    )

    def lay(column):
        return jnp.sum(jnp.where(diagonal, column, 0.0), axis=0, keepdims=True)

    part1[0] = lay(jnp.sum(gram[...], axis=1, keepdims=True))
    sixth = [
        to_dom(part1.at[0], part1.at[k], gram_send, gram_recv, k - 1, line[k - 1])
        for k in range(1, 8)
    ]
    for copy in sixth:
        copy.start()
    for copy in sixth:
        copy.wait_recv()
    part2[0] = jnp.sum(part1[...], axis=0)
    seventh = [
        to_dom(part2.at[0], part2.at[k], sum_send, sum_recv, k - 1, far[k - 1])
        for k in range(1, 4)
    ]
    for copy in seventh:
        copy.start()
    for copy in seventh:
        copy.wait_recv()
    total = jnp.sum(part2[...], axis=0) * (1.0 / cells)
    coef[...] = jnp.broadcast_to(
        jnp.sum(jnp.where(diagonal, total, 0.0), axis=1, keepdims=True), (32, 128)
    )
    factors = [jnp.broadcast_to(coef[pl.ds(m, 1), :], (8, 128)) for m in range(32)]

    def project(n, carry):
        l, r = lax.div(n, 8), pl.ds(pl.multiple_of(lax.rem(n, 8) * 8, 8), 8)
        lost = [None, None]
        for j in range(16):
            x = orbs[j // 2, j % 2, l, r, :]
            for i in range(2):
                term = factors[2 * j + i] * x
                lost[i] = term if lost[i] is None else lost[i] + term
        for i in range(2):
            eb[i, l, r, :] = ea[i, l, r, :] - lost[i]
        return carry

    lax.fori_loop(0, 64, project, 0)
    store = pltpu.make_async_copy(eb.at[:, pl.ds(0, layers)], out, load_sem.at[0])
    store.start()

    for copy in first + coarse + third + fourth + fifth + sixth + seventh:
        copy.wait_send()
    across.wait_send()
    for n in range(3):

        @pl.when((chip >= n) & (chip < 3))
        def _():
            up(n).wait_send()

        @pl.when((chip <= 3 - n) & (chip > 0))
        def _():
            down(n).wait_send()

    for n in range(1, 4):

        @pl.when(chip >= n)
        def _():
            over_up(n).wait_send()

        @pl.when(chip <= 3 - n)
        def _():
            over_down(n).wait_send()

    store.wait()


def on_device(orbitals, initial_guess, potential, perturbation, level_shifts, assignment):
    cells = orbitals.shape[1] * lax.axis_size("dom") * orbitals.shape[2] * orbitals.shape[3]
    dma = pltpu.SemaphoreType.DMA
    vmem = pltpu.VMEM

    def field(*shape):
        return vmem(shape, F32)

    anywhere = pl.BlockSpec(memory_space=pl.ANY)
    scalars = pl.BlockSpec(memory_space=pltpu.SMEM)
    return pl.pallas_call(
        functools.partial(kernel, cells),
        out_shape=jax.ShapeDtypeStruct(orbitals.shape, F32),
        in_specs=[anywhere] * 4 + [scalars] * 2,
        out_specs=anywhere,
        scratch_shapes=[
            field(8, 2, 8, 64, 128),
            field(2, 10, 64, 128),
            field(8, 64, 128),
            field(8, 64, 128),
            field(2, 2, 64, 128),
            field(2, 96, 128),
            field(2, 96, 128),
            field(16, 128),
            field(6, 16, 128),
            field(2, 2, 2, 64, 128),
            field(2, 2, 2, 64, 128),
            field(2, 10, 64, 128),
            field(2, 10, 64, 128),
            field(2, 12, 64, 128),
            field(2, 12, 64, 128),
            field(8, 32, 128),
            field(8, 32, 128),
            field(8, 32, 128),
            field(10, 32, 128),
            field(16, 128),
            field(6, 16, 128),
            field(6, 64, 128),
            field(32, 128),
            field(8, 1, 128),
            field(4, 1, 128),
            field(32, 128),
            dma((4,)),
            dma((12,)),
            dma((12,)),
            dma((12,)),
            dma((12,)),
            dma((13,)),
            dma((13,)),
            dma((7,)),
            dma((7,)),
            dma((3,)),
            dma((3,)),
        ],
        compiler_params=pltpu.CompilerParams(
            collective_id=0, has_side_effects=True, vmem_limit_bytes=32 << 20
        ),
        name="sternheimer",
    )(orbitals, initial_guess, potential, perturbation, level_shifts, assignment)


def solution(mesh):
    in_specs = (
        P("orb", "dom", None, None),
        P("orb", "dom", None, None),
        P("dom", None, None),
        P("dom", None, None),
        P(),
        P("orb"),
    )
    out_specs = P("orb", "dom", None, None)
    return jax.shard_map(
        on_device, mesh=mesh, in_specs=in_specs, out_specs=out_specs, check_vma=False
    )
```

```python
import functools

import jax
import jax.numpy as jnp
from jax import lax
from jax.experimental import pallas as pl
from jax.experimental.pallas import tpu as pltpu
from jax.sharding import PartitionSpec as P

OMEGA = 0.8
KINETIC = 8.0
MESH = pl.DeviceIdType.MESH
F32 = jnp.float32


def turn(x, shift, axis):
    return pltpu.roll(x, shift % x.shape[axis], axis)


def ring(x, step):
    ya, za = x.ndim - 2, x.ndim - 1
    return (turn(x, 1, ya) + turn(x, -1, ya)) + (turn(x, step, za) + turn(x, -step, za))


def lane_bit(shape, bit):
    return (lax.broadcasted_iota(jnp.int32, shape, len(shape) - 1) & bit) == 0


def pair(first, second, bit):
    za = first.ndim - 1
    return jnp.where(
        lane_bit(first.shape, bit), first + turn(first, -bit, za), second + turn(second, bit, za)
    )


def split(packed, bit):
    za = packed.ndim - 1
    clear = lane_bit(packed.shape, bit)
    return (
        jnp.where(clear, packed, turn(packed, bit, za)),
        jnp.where(clear, turn(packed, -bit, za), packed),
    )


def kernel(
    cells, orb_in, guess_in, pot_in, pert_in, table, slot, out,
    orbs, g, pot, pert, gh, st_out, st_in, c2_out, c2_in, fe_out, fe_in,
    f, w, ea, eb, f1, c1, w1, e1, f2_out, f2_in, rows, gram, part, coef,
    load_sem, halo_send, halo_recv, wide_send, wide_recv, ag_send, ag_recv,
    gram_send, gram_recv,
):
    d = lax.axis_index("dom")
    o = lax.axis_index("orb")
    doms = lax.axis_size("dom")
    layers, half, quarter = 8, 4, 2

    loads = [
        pltpu.make_async_copy(guess_in, g.at[:, pl.ds(1, layers)], load_sem.at[0]),
        pltpu.make_async_copy(orb_in, orbs.at[o], load_sem.at[1]),
        pltpu.make_async_copy(pot_in, pot, load_sem.at[2]),
        pltpu.make_async_copy(pert_in, pert, load_sem.at[3]),
    ]
    for copy in loads:
        copy.start()

    barrier = pltpu.get_barrier_semaphore()
    near = [lax.rem(d + doms + k, doms) for k in (-3, -2, -1, 1, 2, 3)]
    rest = [lax.rem(d + k, doms) for k in range(1, doms)]
    chip, core = lax.div(o, 2), lax.rem(o, 2)
    mate = o + 1 - 2 * core
    others = [mate] + [lax.rem(o + 2 * k, 8) for k in range(1, 4)]
    for there in rest:
        pl.semaphore_signal(barrier, inc=1, device_id={"dom": there}, device_id_type=MESH)
    for there in others:
        pl.semaphore_signal(barrier, inc=1, device_id={"orb": there}, device_id_type=MESH)

    shift = [table[slot[i]] for i in range(2)]
    base = [6.0 * KINETIC + s for s in shift]
    zero = jnp.zeros((64, 128), F32)
    for i in range(2):
        g[i, 0] = zero
        g[i, layers + 1] = zero
    for copy in loads:
        copy.wait()

    def start_layer(l, carry):
        p, q = pot[l], pert[l]
        for i in range(2):
            x = g[i, l + 1]
            diag = p + base[i]
            around = ring(x, 1) + (g[i, l] + g[i, l + 2])
            f[i, l + 1] = KINETIC * around - diag * x - q * orbs[o, i, l]
            w[i, l + 1] = OMEGA / diag
        return carry

    lax.fori_loop(0, layers, start_layer, 0)
    for side, (edge, inner) in enumerate(((1, 2), (layers, layers - 1))):
        for i in range(2):
            fe_out[side, 0, i] = f[i, edge]
            fe_out[side, 1, i] = w[i, inner] * f[i, inner]

    for q in range(half):
        t = pot[2 * q] + pot[2 * q + 1]
        rows[q] = pair(t, t, 1)
    for q in range(half):
        c1[q + 2] = 0.125 * (rows[q, pl.ds(0, 32, stride=2)] + rows[q, pl.ds(1, 32, stride=2)])
    even = lane_bit((32, 128), 1)
    st_out[0, pl.ds(0, 64)] = pot[0]
    st_out[1, pl.ds(0, 64)] = pot[layers - 1]
    st_out[0, pl.ds(64, 32)] = jnp.where(even, c1[2], c1[3])
    st_out[1, pl.ds(64, 32)] = jnp.where(even, c1[4], c1[5])
    for q in range(quarter):
        t = c1[2 * q + 2] + c1[2 * q + 3]
        rows[q, pl.ds(0, 32)] = pair(t, t, 2)
    c2 = [
        0.125 * (rows[q, pl.ds(0, 16, stride=2)] + rows[q, pl.ds(1, 16, stride=2)])
        for q in range(quarter)
    ]
    low = lane_bit((16, 128), 2)
    c2_out[...] = jnp.where(low, c2[0], c2[1])

    pl.semaphore_wait(barrier, len(rest) + len(others))

    def to_dom(src, dst, sends, recvs, k, there):
        return pltpu.make_async_remote_copy(
            src_ref=src, dst_ref=dst, send_sem=sends.at[k], recv_sem=recvs.at[k],
            device_id={"dom": there}, device_id_type=MESH,
        )

    below, above = near[2], near[3]
    first = []
    for side, there in ((0, below), (1, above)):
        edge = 1 if side == 0 else layers
        first += [
            to_dom(fe_out.at[side], fe_in.at[1 - side], halo_send, halo_recv, side, there),
            to_dom(g.at[:, edge], gh.at[1 - side], halo_send, halo_recv, 2 + side, there),
        ]
    ahead = 1 - 2 * core
    static = [
        to_dom(
            st_out.at[1 - core], st_in.at[core], halo_send, halo_recv, 4,
            lax.rem(d + doms + ahead, doms),
        )
    ]
    for n in range(1, 4):
        place = core * (2 + n) + (1 - core) * (3 - n)
        static.append(
            to_dom(
                c2_out, c2_in.at[place], wide_send, wide_recv, n,
                lax.rem(d + doms + n * ahead, doms),
            )
        )
    for copy in static[:1] + first + static[1:]:
        copy.start()

    pair_side, odd = lax.div(chip, 2), lax.rem(chip, 2)
    partner = 2 * (chip + 1 - 2 * odd) + core
    across_inner = 2 * (2 - pair_side) + core
    across_outer = 2 * (3 - 3 * pair_side) + core
    blocks = [partner, across_inner, across_outer]
    is_inner = (chip == 1) | (chip == 2)
    is_outer = (chip == 0) | (chip == 3)

    def hand(block, send, recv, there):
        return pltpu.make_async_remote_copy(
            src_ref=orbs.at[block], dst_ref=orbs.at[block],
            send_sem=ag_send.at[send], recv_sem=ag_recv.at[recv],
            device_id={"orb": there}, device_id_type=MESH,
        )

    to_mate = hand(o, 0, 3, mate)
    to_partner = hand(o, 1, 0, partner)
    inner_sends = [hand(o, 2, 1, across_outer), hand(o, 3, 1, across_inner)]
    outer_sends = [hand(o, 2, 2, across_inner)]
    relayed = hand(across_outer, 4, 2, partner)
    taken = [hand(blocks[t], 5 + t, t, mate) for t in range(3)]
    passed = [hand(blocks[t], 5 + t, 4 + t, mate) for t in range(3)]

    @pl.when(is_outer)
    def _():
        outer_sends[0].start()

    @pl.when(is_inner)
    def _():
        inner_sends[0].start()

    to_partner.start()

    @pl.when(is_inner)
    def _():
        inner_sends[1].start()

    to_mate.start()

    static[0].wait_recv()
    swap = [
        pltpu.make_async_remote_copy(
            src_ref=st_in.at[core], dst_ref=st_in.at[core],
            send_sem=halo_send.at[5], recv_sem=halo_recv.at[5],
            device_id={"orb": mate}, device_id_type=MESH,
        )
    ]
    swap[0].start()
    for copy in first:
        copy.wait_recv()

    swap[0].wait_recv()

    for i in range(2):
        f[i, 1] = f[i, 1] + KINETIC * gh[0, i]
        f[i, layers] = f[i, layers] + KINETIC * gh[1, i]
        for side, (beyond, edge, rim) in enumerate(((0, 1, 0), (layers + 1, layers, 11))):
            f[i, beyond] = fe_in[side, 0, i] + KINETIC * g[i, edge]
            w[i, beyond] = OMEGA / (st_in[side, pl.ds(0, 64)] + base[i])
            ea[i, rim] = fe_in[side, 1, i]
    c1[0], c1[1] = split(st_in[0, pl.ds(64, 32)], 1)
    c1[6], c1[7] = split(st_in[1, pl.ds(64, 32)], 1)

    def begin(l, carry):
        for i in range(2):
            ea[i, l + 1] = w[i, l] * f[i, l]
        return carry

    lax.fori_loop(0, layers + 2, begin, 0)

    def sweep_down(l, carry):
        for i in range(2):
            around = ring(ea[i, l + 1], 1) + (ea[i, l] + ea[i, l + 2])
            eb[i, l + 1] = w[i, l] * ((2.0 - OMEGA) * f[i, l] + KINETIC * around)
        return carry

    lax.fori_loop(0, layers + 2, sweep_down, 0)
    second = [
        to_dom(eb.at[:, 3], eb.at[:, 11], halo_send, halo_recv, 6, below),
        to_dom(eb.at[:, 8], eb.at[:, 0], halo_send, halo_recv, 7, above),
    ]

    def remainder(q, carry):
        total = []
        for i in range(2):
            parts = []
            for h in range(2):
                l = 2 * q + h
                x = eb[i, l + 2]
                around = ring(x, 1) + (eb[i, l + 1] + eb[i, l + 3])
                parts.append(f[i, l + 1] + KINETIC * around - (pot[l] + base[i]) * x)
            total.append(parts[0] + parts[1])
        rows[q] = pair(total[0], total[1], 1)
        return carry

    lax.fori_loop(0, half, remainder, 0)
    for q in range(half):
        f1[q + 2] = 0.125 * (rows[q, pl.ds(0, 32, stride=2)] + rows[q, pl.ds(1, 32, stride=2)])
    third = [
        to_dom(f1.at[pl.ds(2, 2)], f1.at[pl.ds(6, 2)], halo_send, halo_recv, 8, below),
        to_dom(f1.at[pl.ds(4, 2)], f1.at[pl.ds(0, 2)], halo_send, halo_recv, 9, above),
    ]
    for copy in third + second:
        copy.start()
    for copy in static[1:]:
        copy.wait_recv()
    swap.append(
        pltpu.make_async_remote_copy(
            src_ref=c2_in.at[pl.ds(3 * core, 3)], dst_ref=c2_in.at[pl.ds(3 * core, 3)],
            send_sem=wide_send.at[0], recv_sem=wide_recv.at[0],
            device_id={"orb": mate}, device_id_type=MESH,
        )
    )
    swap[1].start()

    k1, k2 = KINETIC / 4, KINETIC / 16
    both = jnp.where(even, shift[0], shift[1])
    for q in range(8):
        w1[q] = OMEGA / (c1[q] + (6.0 * k1 + both))
    swap[1].wait_recv()
    both2 = jnp.where(lane_bit((16, 128), 1), shift[0], shift[1])
    c2s = []
    for k in range(3):
        c2s += split(c2_in[k], 2)
    c2s += c2
    for k in range(3, 6):
        c2s += split(c2_in[k], 2)
    w2 = jnp.stack([OMEGA / (c + (6.0 * k2 + both2)) for c in c2s[1:13]])

    for copy in third:
        copy.wait_recv()
    fs, ws = f1[...], w1[...]
    e = ws * fs
    e = ws[1:7] * ((2.0 - OMEGA) * fs[1:7] + k1 * (ring(e[1:7], 2) + (e[:6] + e[2:])))
    e1[pl.ds(2, 6)] = e
    x = e[1:5]
    r = fs[2:6] + k1 * (ring(x, 2) + (e[:4] + e[2:])) - (c1[pl.ds(2, 4)] + (6.0 * k1 + both)) * x
    for q in range(quarter):
        t = r[2 * q] + r[2 * q + 1]
        rows[q, pl.ds(0, 32)] = pair(t, t, 2)
    f2 = [
        0.125 * (rows[q, pl.ds(0, 16, stride=2)] + rows[q, pl.ds(1, 16, stride=2)])
        for q in range(quarter)
    ]
    f2_out[...] = jnp.where(low, f2[0], f2[1])
    fourth = [
        to_dom(f2_out, f2_in.at[5 - k], wide_send, wide_recv, 6 + k, near[k]) for k in range(6)
    ]
    fifth = [
        to_dom(e1.at[pl.ds(4, 2)], e1.at[pl.ds(8, 2)], halo_send, halo_recv, 10, below),
        to_dom(e1.at[pl.ds(4, 2)], e1.at[pl.ds(0, 2)], halo_send, halo_recv, 11, above),
    ]
    for copy in fourth + fifth:
        copy.start()
    @pl.when(is_inner)
    def _():
        taken[2].wait_recv()
        relayed.start()
        passed[2].start()

    for copy in fourth:
        copy.wait_recv()

    f2s = []
    for k in range(3):
        f2s += split(f2_in[k], 2)
    f2s += f2
    for k in range(3, 6):
        f2s += split(f2_in[k], 2)
    f2v = jnp.stack(f2s[1:13])
    e = w2 * f2v
    for n in range(1, 4):
        inner = slice(n, 12 - n)
        x = e[1:-1]
        e = (1.0 - OMEGA) * x + w2[inner] * (f2v[inner] + k2 * (ring(x, 4) + (e[:-2] + e[2:])))

    for q in range(6):
        rows[q, pl.ds(0, 16, stride=2)] = e[q]
        rows[q, pl.ds(1, 16, stride=2)] = e[q]
    for copy in fifth:
        copy.wait_recv()
    e = jnp.stack([e1[l + 3] + rows[l // 2 + 2, pl.ds(0, 32)] for l in range(-3, 7)])
    for n in range(2):
        inner = slice(n, 8 - n)
        x = e[1:-1]
        e = (1.0 - OMEGA) * x + ws[inner] * (fs[inner] + k1 * (ring(x, 2) + (e[:-2] + e[2:])))
    for q in range(6):
        rows[q, pl.ds(0, 32, stride=2)] = e[q]
        rows[q, pl.ds(1, 32, stride=2)] = e[q]

    for copy in second:
        copy.wait_recv()

    def correct(q, carry):
        fields = split(rows[q], 1)
        for i in range(2):
            for h in range(2):
                ea[i, 2 * q + h] = eb[i, 2 * q + h] + fields[i]
        return carry

    lax.fori_loop(0, 6, correct, 0)
    for copy in second:
        copy.wait_send()

    def sweep_up(l, carry):
        for i in range(2):
            x = ea[i, l + 1]
            around = ring(x, 1) + (ea[i, l] + ea[i, l + 2])
            eb[i, l + 1] = (1.0 - OMEGA) * x + w[i, l] * (f[i, l] + KINETIC * around)
        return carry

    lax.fori_loop(0, layers + 2, sweep_up, 0)

    def sweep_last(l, carry):
        for i in range(2):
            x = eb[i, l + 2]
            around = ring(x, 1) + (eb[i, l + 1] + eb[i, l + 3])
            ea[i, l] = g[i, l + 1] + (
                (1.0 - OMEGA) * x + w[i, l + 1] * (f[i, l + 1] + KINETIC * around)
            )
        return carry

    lax.fori_loop(0, layers, sweep_last, 0)

    def intersect(q):
        def products(n, sums):
            l, r = lax.div(n, 8), pl.ds(pl.multiple_of(lax.rem(n, 8) * 8, 8), 8)
            u = [ea[i, l, r, :] for i in range(2)]
            new = []
            for j in range(4):
                x = orbs[2 * q + j // 2, j % 2, l, r, :]
                new += [sums[2 * j + i] + x * u[i] for i in range(2)]
            return tuple(new)

        sums = lax.fori_loop(0, 64, products, (jnp.zeros((8, 128), F32),) * 8, unroll=4)
        for m in range(8):
            gram[q, pl.ds(m, 1), :] = jnp.sum(sums[m], axis=0, keepdims=True)

    for t in range(2):
        taken[t].wait_recv()
        passed[t].start()
    to_mate.wait_recv()
    intersect(chip)
    for t in range(2):
        passed[t].wait_recv()
        intersect(lax.div(blocks[t], 2))

    @pl.when(is_outer)
    def _():
        taken[2].wait_recv()
        passed[2].start()

    passed[2].wait_recv()
    intersect(lax.div(blocks[2], 2))
    diagonal = lax.broadcasted_iota(jnp.int32, (32, 128), 0) == lax.broadcasted_iota(
        jnp.int32, (32, 128), 1
    )

    def lay(column):
        return jnp.sum(jnp.where(diagonal, column, 0.0), axis=0, keepdims=True)

    part[0] = lay(jnp.sum(gram[...].reshape(32, 128), axis=1, keepdims=True))
    sixth = [
        to_dom(part.at[0], part.at[k], gram_send, gram_recv, k - 1, rest[k - 1])
        for k in range(1, doms)
    ]
    for copy in sixth:
        copy.start()
    for copy in sixth:
        copy.wait_recv()
    total = jnp.sum(part[...], axis=0) * (1.0 / cells)
    coef[...] = jnp.broadcast_to(
        jnp.sum(jnp.where(diagonal, total, 0.0), axis=1, keepdims=True), (32, 128)
    )
    factors = [jnp.broadcast_to(coef[pl.ds(m, 1), :], (8, 128)) for m in range(32)]

    def project(n, carry):
        l, r = lax.div(n, 8), pl.ds(pl.multiple_of(lax.rem(n, 8) * 8, 8), 8)
        lost = [None, None]
        for j in range(16):
            x = orbs[j // 2, j % 2, l, r, :]
            for i in range(2):
                term = factors[2 * j + i] * x
                lost[i] = term if lost[i] is None else lost[i] + term
        for i in range(2):
            eb[i, l, r, :] = ea[i, l, r, :] - lost[i]
        return carry

    lax.fori_loop(0, 64, project, 0)
    store = pltpu.make_async_copy(eb.at[:, pl.ds(0, layers)], out, load_sem.at[0])
    store.start()

    for copy in first + static + swap + third + fourth + fifth + sixth:
        copy.wait_send()
    for copy in [to_mate, to_partner] + passed:
        copy.wait_send()

    @pl.when(is_outer)
    def _():
        outer_sends[0].wait_send()

    @pl.when(is_inner)
    def _():
        for copy in inner_sends + [relayed]:
            copy.wait_send()

    store.wait()


def on_device(orbitals, initial_guess, potential, perturbation, level_shifts, assignment):
    doms = lax.axis_size("dom")
    cells = orbitals.shape[1] * doms * orbitals.shape[2] * orbitals.shape[3]
    dma = pltpu.SemaphoreType.DMA
    vmem = pltpu.VMEM

    def field(*shape):
        return vmem(shape, F32)

    anywhere = pl.BlockSpec(memory_space=pltpu.HBM)
    scalars = pl.BlockSpec(memory_space=pltpu.SMEM)
    return pl.pallas_call(
        functools.partial(kernel, cells),
        out_shape=jax.ShapeDtypeStruct(orbitals.shape, F32),
        in_specs=[anywhere] * 4 + [scalars] * 2,
        out_specs=anywhere,
        scratch_shapes=[
            field(8, 2, 8, 64, 128),
            field(2, 10, 64, 128),
            field(8, 64, 128),
            field(8, 64, 128),
            field(2, 2, 64, 128),
            field(2, 96, 128),
            field(2, 96, 128),
            field(16, 128),
            field(6, 16, 128),
            field(2, 2, 2, 64, 128),
            field(2, 2, 2, 64, 128),
            field(2, 10, 64, 128),
            field(2, 10, 64, 128),
            field(2, 12, 64, 128),
            field(2, 12, 64, 128),
            field(8, 32, 128),
            field(8, 32, 128),
            field(8, 32, 128),
            field(10, 32, 128),
            field(16, 128),
            field(6, 16, 128),
            field(6, 64, 128),
            field(4, 8, 128),
            field(doms, 1, 128),
            field(32, 128),
            dma((4,)),
            dma((12,)),
            dma((12,)),
            dma((12,)),
            dma((12,)),
            dma((8,)),
            dma((7,)),
            dma((doms - 1,)),
            dma((doms - 1,)),
        ],
        compiler_params=pltpu.CompilerParams(
            collective_id=0, has_side_effects=True, vmem_limit_bytes=67043328
        ),
        name="sternheimer",
    )(orbitals, initial_guess, potential, perturbation, level_shifts, assignment)


def solution(mesh):
    in_specs = (
        P("orb", "dom", None, None),
        P("orb", "dom", None, None),
        P("dom", None, None),
        P("dom", None, None),
        P(),
        P("orb"),
    )
    out_specs = P("orb", "dom", None, None)
    return jax.shard_map(
        on_device, mesh=mesh, in_specs=in_specs, out_specs=out_specs, check_vma=False
    )
```

```python
import functools

import jax
import jax.numpy as jnp
from jax import lax
from jax.experimental import pallas as pl
from jax.experimental.pallas import tpu as pltpu
from jax.sharding import PartitionSpec as P

OMEGA = 0.8
KINETIC = 8.0
MESH = pl.DeviceIdType.MESH
F32 = jnp.float32


def turn(x, shift, axis):
    return pltpu.roll(x, shift % x.shape[axis], axis)


def ring(x, step):
    ya, za = x.ndim - 2, x.ndim - 1
    return (turn(x, 1, ya) + turn(x, -1, ya)) + (turn(x, step, za) + turn(x, -step, za))


def lane_bit(shape, bit):
    return (lax.broadcasted_iota(jnp.int32, shape, len(shape) - 1) & bit) == 0


def pair(first, second, bit):
    za = first.ndim - 1
    return jnp.where(
        lane_bit(first.shape, bit), first + turn(first, -bit, za), second + turn(second, bit, za)
    )


def split(packed, bit):
    za = packed.ndim - 1
    clear = lane_bit(packed.shape, bit)
    return (
        jnp.where(clear, packed, turn(packed, bit, za)),
        jnp.where(clear, turn(packed, -bit, za), packed),
    )


def kernel(
    cells, orb_in, guess_in, pot_in, pert_in, table_in, slot_in, out,
    orbs, g, pot, pert, gh, st_out, st_in, c2_out, c2_in, fe_out, fe_in,
    f, w, ea, eb, f1, c1, w1, e1, f2_out, f2_in, rows, gram, guest, part, coef,
    table, slot, load_sem, halo_send, halo_recv, wide_send, wide_recv, ag_send, ag_recv,
    gram_send, gram_recv,
):
    d = lax.axis_index("dom")
    o = lax.axis_index("orb")
    doms = lax.axis_size("dom")
    layers, half, quarter = 8, 4, 2

    barrier = pltpu.get_barrier_semaphore()
    near = [lax.rem(d + doms + k, doms) for k in (-3, -2, -1, 1, 2, 3)]
    rest = [lax.rem(d + k, doms) for k in range(1, doms)]
    chip, core = lax.div(o, 2), lax.rem(o, 2)
    mate = o + 1 - 2 * core
    others = [mate] + [lax.rem(o + 2 * k, 8) for k in range(1, 4)]
    for there in rest:
        pl.semaphore_signal(barrier, inc=1, device_id={"dom": there}, device_id_type=MESH)
    for there in others:
        pl.semaphore_signal(barrier, inc=1, device_id={"orb": there}, device_id_type=MESH)

    loads = [
        pltpu.make_async_copy(guess_in, g.at[:, pl.ds(1, layers)], load_sem.at[0]),
        pltpu.make_async_copy(orb_in, orbs.at[o], load_sem.at[1]),
        pltpu.make_async_copy(pot_in, pot, load_sem.at[2]),
        pltpu.make_async_copy(pert_in, pert, load_sem.at[3]),
        pltpu.make_async_copy(table_in, table, load_sem.at[4]),
        pltpu.make_async_copy(slot_in, slot, load_sem.at[5]),
    ]
    for copy in loads:
        copy.start()
    zero = jnp.zeros((64, 128), F32)
    for i in range(2):
        g[i, 0] = zero
        g[i, layers + 1] = zero
    for copy in loads:
        copy.wait()
    shift = [table[slot[i]] for i in range(2)]
    base = [6.0 * KINETIC + s for s in shift]

    def start_layer(l, carry):
        p, q = pot[l], pert[l]
        for i in range(2):
            x = g[i, l + 1]
            diag = p + base[i]
            around = ring(x, 1) + (g[i, l] + g[i, l + 2])
            f[i, l + 1] = KINETIC * around - diag * x - q * orbs[o, i, l]
            w[i, l + 1] = OMEGA / diag
        return carry

    lax.fori_loop(0, layers, start_layer, 0)
    for side, (edge, inner) in enumerate(((1, 2), (layers, layers - 1))):
        for i in range(2):
            fe_out[side, 0, i] = f[i, edge]
            fe_out[side, 1, i] = w[i, inner] * f[i, inner]

    for q in range(half):
        t = pot[2 * q] + pot[2 * q + 1]
        rows[q] = pair(t, t, 1)
    for q in range(half):
        c1[q + 2] = 0.125 * (rows[q, pl.ds(0, 32, stride=2)] + rows[q, pl.ds(1, 32, stride=2)])
    even = lane_bit((32, 128), 1)
    st_out[0, pl.ds(0, 64)] = pot[0]
    st_out[1, pl.ds(0, 64)] = pot[layers - 1]
    st_out[0, pl.ds(64, 32)] = jnp.where(even, c1[2], c1[3])
    st_out[1, pl.ds(64, 32)] = jnp.where(even, c1[4], c1[5])
    for q in range(quarter):
        t = c1[2 * q + 2] + c1[2 * q + 3]
        rows[q, pl.ds(0, 32)] = pair(t, t, 2)
    c2 = [
        0.125 * (rows[q, pl.ds(0, 16, stride=2)] + rows[q, pl.ds(1, 16, stride=2)])
        for q in range(quarter)
    ]
    low = lane_bit((16, 128), 2)
    c2_out[...] = jnp.where(low, c2[0], c2[1])

    pl.semaphore_wait(barrier, len(rest) + len(others))

    def to_dom(src, dst, sends, recvs, k, there):
        return pltpu.make_async_remote_copy(
            src_ref=src, dst_ref=dst, send_sem=sends.at[k], recv_sem=recvs.at[k],
            device_id={"dom": there}, device_id_type=MESH,
        )

    below, above = near[2], near[3]
    first = []
    for side, there in ((0, below), (1, above)):
        edge = 1 if side == 0 else layers
        first += [
            to_dom(fe_out.at[side], fe_in.at[1 - side], halo_send, halo_recv, side, there),
            to_dom(g.at[:, edge], gh.at[1 - side], halo_send, halo_recv, 2 + side, there),
        ]
    ahead = 1 - 2 * core
    static = [
        to_dom(
            st_out.at[1 - core], st_in.at[core], halo_send, halo_recv, 4,
            lax.rem(d + doms + ahead, doms),
        )
    ]
    for n in range(1, 4):
        place = core * (2 + n) + (1 - core) * (3 - n)
        static.append(
            to_dom(
                c2_out, c2_in.at[place], wide_send, wide_recv, n,
                lax.rem(d + doms + n * ahead, doms),
            )
        )
    for copy in static[:1] + first + static[1:]:
        copy.start()

    early, late = pl.ds(0, 6), pl.ds(6, 2)
    is_inner = (chip == 1) | (chip == 2)
    is_outer = (chip == 0) | (chip == 3)

    def hand(block, h, k, there, part=pl.ds(0, 8)):
        return pltpu.make_async_remote_copy(
            src_ref=orbs.at[block, h, part], dst_ref=orbs.at[block, h, part],
            send_sem=ag_send.at[k], recv_sem=ag_recv.at[k],
            device_id={"orb": there}, device_id_type=MESH,
        )

    def reach(n, most):
        return early if n == most else pl.ds(0, 8)

    def up(n, h):
        return hand(o - 2 * n, h, 2 * n + h, o + 2, reach(n, 2))

    def down(n, h):
        return hand(o + 2 * n, h, 6 + 2 * n + h, o - 2, reach(n, 2))

    def share_up(n, h):
        return hand(o - 2 * n, h, 12 + 2 * n + h, mate, reach(n, 3))

    def share_down(n, h):
        return hand(o + 2 * n, h, 18 + 2 * n + h, mate, reach(n, 3))

    late_up = [hand(o - 4, h, 26 + h, o + 2, late) for h in range(2)]
    late_down = [hand(o + 4, h, 28 + h, o - 2, late) for h in range(2)]
    near_end = o + 2 - 4 * lax.rem(chip, 2)
    far = 2 * (3 - 3 * lax.div(chip, 2)) + core
    late_share = [hand(far, h, 30 + h, mate, late) for h in range(2)]
    visit = pltpu.make_async_remote_copy(
        src_ref=ea.at[:, late], dst_ref=guest,
        send_sem=ag_send.at[32], recv_sem=ag_recv.at[32],
        device_id={"orb": near_end}, device_id_type=MESH,
    )
    answer = pltpu.make_async_remote_copy(
        src_ref=gram.at[4], dst_ref=gram.at[5],
        send_sem=ag_send.at[33], recv_sem=ag_recv.at[33],
        device_id={"orb": near_end}, device_id_type=MESH,
    )
    own = [hand(o, h, 12 + h, mate) for h in range(2)]

    def relay(n, h):
        @pl.when(chip >= n)
        def _():
            hand(o - 2 * n, h, 2 * (n - 1) + h, mate, reach(n, 3)).wait_recv()
            if n < 3:

                @pl.when(chip < 3)
                def _():
                    up(n, h).start()

            share_up(n, h).start()

        @pl.when(chip <= 3 - n)
        def _():
            hand(o + 2 * n, h, 6 + 2 * (n - 1) + h, mate, reach(n, 3)).wait_recv()
            if n < 3:

                @pl.when(chip > 0)
                def _():
                    down(n, h).start()

            share_down(n, h).start()

    for h in range(2):

        @pl.when(chip < 3)
        def _():
            up(0, h).start()

        @pl.when(chip > 0)
        def _():
            down(0, h).start()

    for copy in own:
        copy.start()

    static[0].wait_recv()
    swap = [
        pltpu.make_async_remote_copy(
            src_ref=st_in.at[core], dst_ref=st_in.at[core],
            send_sem=halo_send.at[5], recv_sem=halo_recv.at[5],
            device_id={"orb": mate}, device_id_type=MESH,
        )
    ]
    swap[0].start()
    for copy in first:
        copy.wait_recv()

    swap[0].wait_recv()

    for i in range(2):
        f[i, 1] = f[i, 1] + KINETIC * gh[0, i]
        f[i, layers] = f[i, layers] + KINETIC * gh[1, i]
        for side, (beyond, edge, rim) in enumerate(((0, 1, 0), (layers + 1, layers, 11))):
            f[i, beyond] = fe_in[side, 0, i] + KINETIC * g[i, edge]
            w[i, beyond] = OMEGA / (st_in[side, pl.ds(0, 64)] + base[i])
            ea[i, rim] = fe_in[side, 1, i]
    c1[0], c1[1] = split(st_in[0, pl.ds(64, 32)], 1)
    c1[6], c1[7] = split(st_in[1, pl.ds(64, 32)], 1)

    def begin(l, carry):
        for i in range(2):
            ea[i, l + 1] = w[i, l] * f[i, l]
        return carry

    lax.fori_loop(0, layers + 2, begin, 0)

    def sweep_down(l, carry):
        for i in range(2):
            around = ring(ea[i, l + 1], 1) + (ea[i, l] + ea[i, l + 2])
            eb[i, l + 1] = w[i, l] * ((2.0 - OMEGA) * f[i, l] + KINETIC * around)
        return carry

    lax.fori_loop(0, layers + 2, sweep_down, 0)
    second = [
        to_dom(eb.at[:, 3], eb.at[:, 11], halo_send, halo_recv, 6, below),
        to_dom(eb.at[:, 8], eb.at[:, 0], halo_send, halo_recv, 7, above),
    ]

    def remainder(q, carry):
        total = []
        for i in range(2):
            parts = []
            for h in range(2):
                l = 2 * q + h
                x = eb[i, l + 2]
                around = ring(x, 1) + (eb[i, l + 1] + eb[i, l + 3])
                parts.append(f[i, l + 1] + KINETIC * around - (pot[l] + base[i]) * x)
            total.append(parts[0] + parts[1])
        rows[q] = pair(total[0], total[1], 1)
        return carry

    lax.fori_loop(0, half, remainder, 0)
    for q in range(half):
        f1[q + 2] = 0.125 * (rows[q, pl.ds(0, 32, stride=2)] + rows[q, pl.ds(1, 32, stride=2)])
    third = [
        to_dom(f1.at[pl.ds(2, 2)], f1.at[pl.ds(6, 2)], halo_send, halo_recv, 8, below),
        to_dom(f1.at[pl.ds(4, 2)], f1.at[pl.ds(0, 2)], halo_send, halo_recv, 9, above),
    ]
    for copy in third + second:
        copy.start()
    for copy in static[1:]:
        copy.wait_recv()
    swap.append(
        pltpu.make_async_remote_copy(
            src_ref=c2_in.at[pl.ds(3 * core, 3)], dst_ref=c2_in.at[pl.ds(3 * core, 3)],
            send_sem=wide_send.at[0], recv_sem=wide_recv.at[0],
            device_id={"orb": mate}, device_id_type=MESH,
        )
    )
    swap[1].start()

    k1, k2 = KINETIC / 4, KINETIC / 16
    both = jnp.where(even, shift[0], shift[1])
    for q in range(8):
        w1[q] = OMEGA / (c1[q] + (6.0 * k1 + both))
    swap[1].wait_recv()
    both2 = jnp.where(lane_bit((16, 128), 1), shift[0], shift[1])
    c2s = []
    for k in range(3):
        c2s += split(c2_in[k], 2)
    c2s += c2
    for k in range(3, 6):
        c2s += split(c2_in[k], 2)
    w2 = jnp.stack([OMEGA / (c + (6.0 * k2 + both2)) for c in c2s[1:13]])

    for copy in third:
        copy.wait_recv()
    fs, ws = f1[...], w1[...]
    e = ws * fs
    e = ws[1:7] * ((2.0 - OMEGA) * fs[1:7] + k1 * (ring(e[1:7], 2) + (e[:6] + e[2:])))
    e1[pl.ds(2, 6)] = e
    x = e[1:5]
    r = fs[2:6] + k1 * (ring(x, 2) + (e[:4] + e[2:])) - (c1[pl.ds(2, 4)] + (6.0 * k1 + both)) * x
    for q in range(quarter):
        t = r[2 * q] + r[2 * q + 1]
        rows[q, pl.ds(0, 32)] = pair(t, t, 2)
    f2 = [
        0.125 * (rows[q, pl.ds(0, 16, stride=2)] + rows[q, pl.ds(1, 16, stride=2)])
        for q in range(quarter)
    ]
    f2_out[...] = jnp.where(low, f2[0], f2[1])
    fourth = [
        to_dom(f2_out, f2_in.at[5 - k], wide_send, wide_recv, 6 + k, near[k]) for k in range(6)
    ]
    fifth = [
        to_dom(e1.at[pl.ds(4, 2)], e1.at[pl.ds(8, 2)], halo_send, halo_recv, 10, below),
        to_dom(e1.at[pl.ds(4, 2)], e1.at[pl.ds(0, 2)], halo_send, halo_recv, 11, above),
    ]
    for copy in fourth + fifth:
        copy.start()
    relay(1, 0)
    relay(1, 1)
    for copy in fourth:
        copy.wait_recv()

    f2s = []
    for k in range(3):
        f2s += split(f2_in[k], 2)
    f2s += f2
    for k in range(3, 6):
        f2s += split(f2_in[k], 2)
    f2v = jnp.stack(f2s[1:13])
    e = w2 * f2v
    for n in range(1, 4):
        inner = slice(n, 12 - n)
        x = e[1:-1]
        e = (1.0 - OMEGA) * x + w2[inner] * (f2v[inner] + k2 * (ring(x, 4) + (e[:-2] + e[2:])))

    for q in range(6):
        rows[q, pl.ds(0, 16, stride=2)] = e[q]
        rows[q, pl.ds(1, 16, stride=2)] = e[q]
    for copy in fifth:
        copy.wait_recv()
    e = jnp.stack([e1[l + 3] + rows[l // 2 + 2, pl.ds(0, 32)] for l in range(-3, 7)])
    for n in range(2):
        inner = slice(n, 8 - n)
        x = e[1:-1]
        e = (1.0 - OMEGA) * x + ws[inner] * (fs[inner] + k1 * (ring(x, 2) + (e[:-2] + e[2:])))
    for q in range(6):
        rows[q, pl.ds(0, 32, stride=2)] = e[q]
        rows[q, pl.ds(1, 32, stride=2)] = e[q]

    relay(2, 0)

    for copy in second:
        copy.wait_recv()

    def correct(q, carry):
        fields = split(rows[q], 1)
        for i in range(2):
            for h in range(2):
                ea[i, 2 * q + h] = eb[i, 2 * q + h] + fields[i]
        return carry

    lax.fori_loop(0, 6, correct, 0)
    for copy in second:
        copy.wait_send()

    def sweep_up(l, carry):
        for i in range(2):
            x = ea[i, l + 1]
            around = ring(x, 1) + (ea[i, l] + ea[i, l + 2])
            eb[i, l + 1] = (1.0 - OMEGA) * x + w[i, l] * (f[i, l] + KINETIC * around)
        return carry

    lax.fori_loop(0, layers + 2, sweep_up, 0)

    def sweep_last(l, carry):
        for i in range(2):
            x = eb[i, l + 2]
            around = ring(x, 1) + (eb[i, l + 1] + eb[i, l + 3])
            ea[i, l] = g[i, l + 1] + (
                (1.0 - OMEGA) * x + w[i, l + 1] * (f[i, l + 1] + KINETIC * around)
            )
        return carry

    lax.fori_loop(layers - 2, layers, sweep_last, 0)

    @pl.when(is_outer)
    def _():
        visit.start()

    lax.fori_loop(0, layers - 2, sweep_last, 0)
    relay(2, 1)

    def intersect(q, h, start, stop):
        def products(n, sums):
            l, r = lax.div(n, 8), pl.ds(pl.multiple_of(lax.rem(n, 8) * 8, 8), 8)
            u = [ea[i, l, r, :] for i in range(2)]
            new = []
            for c in range(2):
                x = orbs[2 * q + c, h, l, r, :]
                new += [sums[2 * c + i] + x * u[i] for i in range(2)]
            return tuple(new)

        sums = lax.fori_loop(start, stop, products, (jnp.zeros((8, 128), F32),) * 4, unroll=8)
        for m in range(4):
            row = pl.ds(4 * (m // 2) + 2 * h + m % 2, 1)
            found = jnp.sum(sums[m], axis=0, keepdims=True)
            gram[q, row, :] = found

    pair_side, odd = lax.div(chip, 2), lax.rem(chip, 2)
    ways = [
        (chip + 1 - 2 * odd, 1 - odd),
        (2 - pair_side, 1 - pair_side),
        (3 - 3 * pair_side, 1 - pair_side),
    ]
    for copy in own:
        copy.wait_recv()
    for h in range(2):
        intersect(chip, h, 0, 64)
    for n, (q, is_down) in enumerate(ways):
        away = (q - chip) * (2 * is_down - 1)
        slot_of = 12 + 6 * is_down + 2 * away
        block = 2 * q + 1 - core
        for h in range(2):
            if n < 2:
                hand(block, h, slot_of + h, mate).wait_recv()
                intersect(q, h, 0, 64)
                continue
            relay(3, h)

            @pl.when(is_outer)
            def _():
                hand(block, h, slot_of + h, mate, early).wait_recv()

            @pl.when(is_inner)
            def _():
                hand(block, h, slot_of + h, mate).wait_recv()
                intersect(q, h, 0, 64)

            @pl.when(is_outer)
            def _():
                intersect(q, h, 0, 48)

    @pl.when(is_inner)
    def _():
        visit.wait_recv()

        def products(n, sums):
            l, r = lax.div(n, 8), pl.ds(pl.multiple_of(lax.rem(n, 8) * 8, 8), 8)
            u = [guest[i, l, r, :] for i in range(2)]
            new = []
            for c in range(2):
                for h in range(2):
                    x = orbs[far - core + c, h, 6 + l, r, :]
                    new += [sums[len(new) + i] + x * u[i] for i in range(2)]
            return tuple(new)

        sums = lax.fori_loop(0, 16, products, (jnp.zeros((8, 128), F32),) * 8, unroll=4)
        for m in range(8):
            gram[4, pl.ds(m, 1), :] = jnp.sum(sums[m], axis=0, keepdims=True)
        answer.start()

    @pl.when(is_outer)
    def _():
        answer.wait_recv()
        last = 3 - 3 * lax.div(chip, 2)
        gram[last] = gram[last] + gram[5]

    diagonal = lax.broadcasted_iota(jnp.int32, (32, 128), 0) == lax.broadcasted_iota(
        jnp.int32, (32, 128), 1
    )

    def lay(column):
        return jnp.sum(jnp.where(diagonal, column, 0.0), axis=0, keepdims=True)

    part[0] = lay(jnp.sum(gram[pl.ds(0, 4)].reshape(32, 128), axis=1, keepdims=True))
    sixth = [
        to_dom(part.at[0], part.at[k], gram_send, gram_recv, k - 1, rest[k - 1])
        for k in range(1, doms)
    ]
    for copy in sixth:
        copy.start()

    @pl.when(chip == 2)
    def _():
        for copy in late_up:
            copy.start()

    @pl.when(chip == 1)
    def _():
        for copy in late_down:
            copy.start()

    for copy in sixth:
        copy.wait_recv()
    total = jnp.sum(part[...], axis=0) * (1.0 / cells)
    coef[...] = jnp.broadcast_to(
        jnp.sum(jnp.where(diagonal, total, 0.0), axis=1, keepdims=True), (32, 128)
    )
    factors = [jnp.broadcast_to(coef[pl.ds(m, 1), :], (8, 128)) for m in range(32)]

    def project(n, carry):
        l, r = lax.div(n, 8), pl.ds(pl.multiple_of(lax.rem(n, 8) * 8, 8), 8)
        lost = [None, None]
        for j in range(16):
            x = orbs[j // 2, j % 2, l, r, :]
            for i in range(2):
                term = factors[2 * j + i] * x
                lost[i] = term if lost[i] is None else lost[i] + term
        for i in range(2):
            eb[i, l, r, :] = ea[i, l, r, :] - lost[i]
        return carry

    for h in range(2):

        @pl.when(chip == 3)
        def _():
            hand(far, h, 26 + h, mate, late).wait_recv()

        @pl.when(chip == 0)
        def _():
            hand(far, h, 28 + h, mate, late).wait_recv()

    @pl.when(is_outer)
    def _():
        for copy in late_share:
            copy.start()

    stores = []
    for k in range(4):
        if k == 3:

            @pl.when(is_outer)
            def _():
                for h in range(2):
                    hand(far + 1 - 2 * core, h, 30 + h, mate, late).wait_recv()

        lax.fori_loop(16 * k, 16 * k + 16, project, 0, unroll=2)
        part_of = pl.ds(2 * k, 2)
        stores.append(pltpu.make_async_copy(eb.at[:, part_of], out.at[:, part_of], load_sem.at[k]))
        stores[k].start()

    for copy in first + static + swap + third + fourth + fifth + sixth:
        copy.wait_send()
    for copy in own:
        copy.wait_send()
    for h in range(2):
        for n in range(3):

            @pl.when((chip >= n) & (chip < 3))
            def _():
                up(n, h).wait_send()

            @pl.when((chip <= 3 - n) & (chip > 0))
            def _():
                down(n, h).wait_send()

        for n in range(1, 4):

            @pl.when(chip >= n)
            def _():
                share_up(n, h).wait_send()

            @pl.when(chip <= 3 - n)
            def _():
                share_down(n, h).wait_send()

    @pl.when(is_outer)
    def _():
        for copy in late_share + [visit]:
            copy.wait_send()

    @pl.when(is_inner)
    def _():
        answer.wait_send()

    @pl.when(chip == 2)
    def _():
        for copy in late_up:
            copy.wait_send()

    @pl.when(chip == 1)
    def _():
        for copy in late_down:
            copy.wait_send()

    for store in stores:
        store.wait()


def on_device(orbitals, initial_guess, potential, perturbation, level_shifts, assignment):
    doms = lax.axis_size("dom")
    cells = orbitals.shape[1] * doms * orbitals.shape[2] * orbitals.shape[3]
    dma = pltpu.SemaphoreType.DMA
    vmem = pltpu.VMEM

    def field(*shape):
        return vmem(shape, F32)

    anywhere = pl.BlockSpec(memory_space=pltpu.HBM)
    return pl.pallas_call(
        functools.partial(kernel, cells),
        out_shape=jax.ShapeDtypeStruct(orbitals.shape, F32),
        in_specs=[anywhere] * 6,
        out_specs=anywhere,
        scratch_shapes=[
            field(8, 2, 8, 64, 128),
            field(2, 10, 64, 128),
            field(8, 64, 128),
            field(8, 64, 128),
            field(2, 2, 64, 128),
            field(2, 96, 128),
            field(2, 96, 128),
            field(16, 128),
            field(6, 16, 128),
            field(2, 2, 2, 64, 128),
            field(2, 2, 2, 64, 128),
            field(2, 10, 64, 128),
            field(2, 10, 64, 128),
            field(2, 12, 64, 128),
            field(2, 12, 64, 128),
            field(8, 32, 128),
            field(8, 32, 128),
            field(8, 32, 128),
            field(10, 32, 128),
            field(16, 128),
            field(6, 16, 128),
            field(6, 64, 128),
            field(6, 8, 128),
            field(2, 2, 64, 128),
            field(doms, 1, 128),
            field(32, 128),
            pltpu.SMEM((16,), F32),
            pltpu.SMEM((2,), jnp.int32),
            dma((6,)),
            dma((12,)),
            dma((12,)),
            dma((12,)),
            dma((12,)),
            dma((34,)),
            dma((34,)),
            dma((doms - 1,)),
            dma((doms - 1,)),
        ],
        compiler_params=pltpu.CompilerParams(
            collective_id=0, has_side_effects=True, vmem_limit_bytes=67043328
        ),
        name="sternheimer",
    )(orbitals, initial_guess, potential, perturbation, level_shifts, assignment)


def solution(mesh):
    in_specs = (
        P("orb", "dom", None, None),
        P("orb", "dom", None, None),
        P("dom", None, None),
        P("dom", None, None),
        P(),
        P("orb"),
    )
    out_specs = P("orb", "dom", None, None)
    return jax.shard_map(
        on_device, mesh=mesh, in_specs=in_specs, out_specs=out_specs, check_vma=False
    )
```

```python
import functools

import jax
import jax.numpy as jnp
from jax import lax
from jax.experimental import pallas as pl
from jax.experimental.pallas import tpu as pltpu
from jax.sharding import PartitionSpec as P

OMEGA = 0.8
LATE = 4
KINETIC = 8.0
MESH = pl.DeviceIdType.MESH
F32 = jnp.float32


def turn(x, shift, axis):
    return pltpu.roll(x, shift % x.shape[axis], axis)


def ring(x, step):
    ya, za = x.ndim - 2, x.ndim - 1
    return (turn(x, 1, ya) + turn(x, -1, ya)) + (turn(x, step, za) + turn(x, -step, za))


def lane_bit(shape, bit):
    return (lax.broadcasted_iota(jnp.int32, shape, len(shape) - 1) & bit) == 0


def pair(first, second, bit):
    za = first.ndim - 1
    return jnp.where(
        lane_bit(first.shape, bit), first + turn(first, -bit, za), second + turn(second, bit, za)
    )


def split(packed, bit):
    za = packed.ndim - 1
    clear = lane_bit(packed.shape, bit)
    return (
        jnp.where(clear, packed, turn(packed, bit, za)),
        jnp.where(clear, turn(packed, -bit, za), packed),
    )


def kernel(
    cells, orb_in, guess_in, pot_in, pert_in, table_in, slot_in, out,
    orbs, g, pot, pert, gh, st_out, st_in, c2_out, c2_in, fe_out, fe_in,
    f, w, ea, eb, f1, c1, w1, e1, f2_out, f2_in, rows, gram, guest, part, coef,
    table, slot, load_sem, halo_send, halo_recv, wide_send, wide_recv, ag_send, ag_recv,
    gram_send, gram_recv,
):
    d = lax.axis_index("dom")
    o = lax.axis_index("orb")
    doms = lax.axis_size("dom")
    layers, half, quarter = 8, 4, 2

    barrier = pltpu.get_barrier_semaphore()
    near = [lax.rem(d + doms + k, doms) for k in (-3, -2, -1, 1, 2, 3)]
    rest = [lax.rem(d + k, doms) for k in range(1, doms)]
    chip, core = lax.div(o, 2), lax.rem(o, 2)
    mate = o + 1 - 2 * core
    others = [mate] + [lax.rem(o + 2 * k, 8) for k in range(1, 4)]
    for there in rest:
        pl.semaphore_signal(barrier, inc=1, device_id={"dom": there}, device_id_type=MESH)
    for there in others:
        pl.semaphore_signal(barrier, inc=1, device_id={"orb": there}, device_id_type=MESH)

    loads = [
        pltpu.make_async_copy(guess_in, g.at[:, pl.ds(1, layers)], load_sem.at[0]),
        pltpu.make_async_copy(orb_in, orbs.at[o], load_sem.at[1]),
        pltpu.make_async_copy(pot_in, pot, load_sem.at[2]),
        pltpu.make_async_copy(pert_in, pert, load_sem.at[3]),
        pltpu.make_async_copy(table_in, table, load_sem.at[4]),
        pltpu.make_async_copy(slot_in, slot, load_sem.at[5]),
    ]
    for copy in loads:
        copy.start()
    zero = jnp.zeros((64, 128), F32)
    for i in range(2):
        g[i, 0] = zero
        g[i, layers + 1] = zero
    for copy in loads:
        copy.wait()
    shift = [table[slot[i]] for i in range(2)]
    base = [6.0 * KINETIC + s for s in shift]

    def start_layer(l, carry):
        p, q = pot[l], pert[l]
        for i in range(2):
            x = g[i, l + 1]
            diag = p + base[i]
            around = ring(x, 1) + (g[i, l] + g[i, l + 2])
            f[i, l + 1] = KINETIC * around - diag * x - q * orbs[o, i, l]
            w[i, l + 1] = OMEGA / diag
        return carry

    lax.fori_loop(0, layers, start_layer, 0)
    for side, (edge, inner) in enumerate(((1, 2), (layers, layers - 1))):
        for i in range(2):
            fe_out[side, 0, i] = f[i, edge]
            fe_out[side, 1, i] = w[i, inner] * f[i, inner]

    for q in range(half):
        t = pot[2 * q] + pot[2 * q + 1]
        rows[q] = pair(t, t, 1)
    for q in range(half):
        c1[q + 2] = 0.125 * (rows[q, pl.ds(0, 32, stride=2)] + rows[q, pl.ds(1, 32, stride=2)])
    even = lane_bit((32, 128), 1)
    st_out[0, pl.ds(0, 64)] = pot[0]
    st_out[1, pl.ds(0, 64)] = pot[layers - 1]
    st_out[0, pl.ds(64, 32)] = jnp.where(even, c1[2], c1[3])
    st_out[1, pl.ds(64, 32)] = jnp.where(even, c1[4], c1[5])
    for q in range(quarter):
        t = c1[2 * q + 2] + c1[2 * q + 3]
        rows[q, pl.ds(0, 32)] = pair(t, t, 2)
    c2 = [
        0.125 * (rows[q, pl.ds(0, 16, stride=2)] + rows[q, pl.ds(1, 16, stride=2)])
        for q in range(quarter)
    ]
    low = lane_bit((16, 128), 2)
    c2_out[...] = jnp.where(low, c2[0], c2[1])

    pl.semaphore_wait(barrier, len(rest) + len(others))

    def to_dom(src, dst, sends, recvs, k, there):
        return pltpu.make_async_remote_copy(
            src_ref=src, dst_ref=dst, send_sem=sends.at[k], recv_sem=recvs.at[k],
            device_id={"dom": there}, device_id_type=MESH,
        )

    below, above = near[2], near[3]
    first = []
    for side, there in ((0, below), (1, above)):
        edge = 1 if side == 0 else layers
        first += [
            to_dom(fe_out.at[side], fe_in.at[1 - side], halo_send, halo_recv, side, there),
            to_dom(g.at[:, edge], gh.at[1 - side], halo_send, halo_recv, 2 + side, there),
        ]
    ahead = 1 - 2 * core
    static = [
        to_dom(
            st_out.at[1 - core], st_in.at[core], halo_send, halo_recv, 4,
            lax.rem(d + doms + ahead, doms),
        )
    ]
    for n in range(1, 4):
        place = core * (2 + n) + (1 - core) * (3 - n)
        static.append(
            to_dom(
                c2_out, c2_in.at[place], wide_send, wide_recv, n,
                lax.rem(d + doms + n * ahead, doms),
            )
        )
    for copy in static[:1] + first + static[1:]:
        copy.start()

    cut = layers - LATE
    early, late = pl.ds(0, cut), pl.ds(cut, LATE)
    is_inner = (chip == 1) | (chip == 2)
    is_outer = (chip == 0) | (chip == 3)

    def hand(block, h, k, there, part=pl.ds(0, 8)):
        return pltpu.make_async_remote_copy(
            src_ref=orbs.at[block, h, part], dst_ref=orbs.at[block, h, part],
            send_sem=ag_send.at[k], recv_sem=ag_recv.at[k],
            device_id={"orb": there}, device_id_type=MESH,
        )

    def reach(n, most):
        return early if n == most else pl.ds(0, 8)

    def up(n, h):
        return hand(o - 2 * n, h, 2 * n + h, o + 2, reach(n, 2))

    def down(n, h):
        return hand(o + 2 * n, h, 6 + 2 * n + h, o - 2, reach(n, 2))

    def share_up(n, h):
        return hand(o - 2 * n, h, 12 + 2 * n + h, mate, reach(n, 3))

    def share_down(n, h):
        return hand(o + 2 * n, h, 18 + 2 * n + h, mate, reach(n, 3))

    late_up = [hand(o - 4, h, 26 + h, o + 2, late) for h in range(2)]
    late_down = [hand(o + 4, h, 28 + h, o - 2, late) for h in range(2)]
    near_end = o + 2 - 4 * lax.rem(chip, 2)
    far = 2 * (3 - 3 * lax.div(chip, 2)) + core
    late_share = [hand(far, h, 30 + h, mate, late) for h in range(2)]
    visit = pltpu.make_async_remote_copy(
        src_ref=ea.at[:, late], dst_ref=guest,
        send_sem=ag_send.at[32], recv_sem=ag_recv.at[32],
        device_id={"orb": near_end}, device_id_type=MESH,
    )
    answer = pltpu.make_async_remote_copy(
        src_ref=gram.at[4], dst_ref=gram.at[5],
        send_sem=ag_send.at[33], recv_sem=ag_recv.at[33],
        device_id={"orb": near_end}, device_id_type=MESH,
    )
    own = [hand(o, h, 12 + h, mate) for h in range(2)]

    def relay(n, h):
        @pl.when(chip >= n)
        def _():
            hand(o - 2 * n, h, 2 * (n - 1) + h, mate, reach(n, 3)).wait_recv()
            if n < 3:

                @pl.when(chip < 3)
                def _():
                    up(n, h).start()

            share_up(n, h).start()

        @pl.when(chip <= 3 - n)
        def _():
            hand(o + 2 * n, h, 6 + 2 * (n - 1) + h, mate, reach(n, 3)).wait_recv()
            if n < 3:

                @pl.when(chip > 0)
                def _():
                    down(n, h).start()

            share_down(n, h).start()

    for h in range(2):

        @pl.when(chip < 3)
        def _():
            up(0, h).start()

        @pl.when(chip > 0)
        def _():
            down(0, h).start()

    for copy in own:
        copy.start()

    static[0].wait_recv()
    swap = [
        pltpu.make_async_remote_copy(
            src_ref=st_in.at[core], dst_ref=st_in.at[core],
            send_sem=halo_send.at[5], recv_sem=halo_recv.at[5],
            device_id={"orb": mate}, device_id_type=MESH,
        )
    ]
    swap[0].start()
    for copy in first:
        copy.wait_recv()

    swap[0].wait_recv()

    for i in range(2):
        f[i, 1] = f[i, 1] + KINETIC * gh[0, i]
        f[i, layers] = f[i, layers] + KINETIC * gh[1, i]
        for side, (beyond, edge, rim) in enumerate(((0, 1, 0), (layers + 1, layers, 11))):
            f[i, beyond] = fe_in[side, 0, i] + KINETIC * g[i, edge]
            w[i, beyond] = OMEGA / (st_in[side, pl.ds(0, 64)] + base[i])
            ea[i, rim] = fe_in[side, 1, i]
    c1[0], c1[1] = split(st_in[0, pl.ds(64, 32)], 1)
    c1[6], c1[7] = split(st_in[1, pl.ds(64, 32)], 1)

    def begin(l, carry):
        for i in range(2):
            ea[i, l + 1] = w[i, l] * f[i, l]
        return carry

    lax.fori_loop(0, layers + 2, begin, 0)

    def sweep_down(l, carry):
        for i in range(2):
            around = ring(ea[i, l + 1], 1) + (ea[i, l] + ea[i, l + 2])
            eb[i, l + 1] = w[i, l] * ((2.0 - OMEGA) * f[i, l] + KINETIC * around)
        return carry

    lax.fori_loop(0, layers + 2, sweep_down, 0)
    second = [
        to_dom(eb.at[:, 3], eb.at[:, 11], halo_send, halo_recv, 6, below),
        to_dom(eb.at[:, 8], eb.at[:, 0], halo_send, halo_recv, 7, above),
    ]

    def remainder(q, carry):
        total = []
        for i in range(2):
            parts = []
            for h in range(2):
                l = 2 * q + h
                x = eb[i, l + 2]
                around = ring(x, 1) + (eb[i, l + 1] + eb[i, l + 3])
                parts.append(f[i, l + 1] + KINETIC * around - (pot[l] + base[i]) * x)
            total.append(parts[0] + parts[1])
        rows[q] = pair(total[0], total[1], 1)
        return carry

    lax.fori_loop(0, half, remainder, 0)
    for q in range(half):
        f1[q + 2] = 0.125 * (rows[q, pl.ds(0, 32, stride=2)] + rows[q, pl.ds(1, 32, stride=2)])
    third = [
        to_dom(f1.at[pl.ds(2, 2)], f1.at[pl.ds(6, 2)], halo_send, halo_recv, 8, below),
        to_dom(f1.at[pl.ds(4, 2)], f1.at[pl.ds(0, 2)], halo_send, halo_recv, 9, above),
    ]
    for copy in third + second:
        copy.start()
    for copy in static[1:]:
        copy.wait_recv()
    swap.append(
        pltpu.make_async_remote_copy(
            src_ref=c2_in.at[pl.ds(3 * core, 3)], dst_ref=c2_in.at[pl.ds(3 * core, 3)],
            send_sem=wide_send.at[0], recv_sem=wide_recv.at[0],
            device_id={"orb": mate}, device_id_type=MESH,
        )
    )
    swap[1].start()

    k1, k2 = KINETIC / 4, KINETIC / 16
    both = jnp.where(even, shift[0], shift[1])
    for q in range(8):
        w1[q] = OMEGA / (c1[q] + (6.0 * k1 + both))
    swap[1].wait_recv()
    both2 = jnp.where(lane_bit((16, 128), 1), shift[0], shift[1])
    c2s = []
    for k in range(3):
        c2s += split(c2_in[k], 2)
    c2s += c2
    for k in range(3, 6):
        c2s += split(c2_in[k], 2)
    w2 = jnp.stack([OMEGA / (c + (6.0 * k2 + both2)) for c in c2s[1:13]])

    for copy in third:
        copy.wait_recv()
    fs, ws = f1[...], w1[...]
    e = ws * fs
    e = ws[1:7] * ((2.0 - OMEGA) * fs[1:7] + k1 * (ring(e[1:7], 2) + (e[:6] + e[2:])))
    e1[pl.ds(2, 6)] = e
    x = e[1:5]
    r = fs[2:6] + k1 * (ring(x, 2) + (e[:4] + e[2:])) - (c1[pl.ds(2, 4)] + (6.0 * k1 + both)) * x
    for q in range(quarter):
        t = r[2 * q] + r[2 * q + 1]
        rows[q, pl.ds(0, 32)] = pair(t, t, 2)
    f2 = [
        0.125 * (rows[q, pl.ds(0, 16, stride=2)] + rows[q, pl.ds(1, 16, stride=2)])
        for q in range(quarter)
    ]
    f2_out[...] = jnp.where(low, f2[0], f2[1])
    fourth = [
        to_dom(f2_out, f2_in.at[5 - k], wide_send, wide_recv, 6 + k, near[k]) for k in range(6)
    ]
    fifth = [
        to_dom(e1.at[pl.ds(4, 2)], e1.at[pl.ds(8, 2)], halo_send, halo_recv, 10, below),
        to_dom(e1.at[pl.ds(4, 2)], e1.at[pl.ds(0, 2)], halo_send, halo_recv, 11, above),
    ]
    for copy in fourth + fifth:
        copy.start()
    relay(1, 0)
    relay(1, 1)
    for copy in fourth:
        copy.wait_recv()

    f2s = []
    for k in range(3):
        f2s += split(f2_in[k], 2)
    f2s += f2
    for k in range(3, 6):
        f2s += split(f2_in[k], 2)
    f2v = jnp.stack(f2s[1:13])
    e = w2 * f2v
    for n in range(1, 4):
        inner = slice(n, 12 - n)
        x = e[1:-1]
        e = (1.0 - OMEGA) * x + w2[inner] * (f2v[inner] + k2 * (ring(x, 4) + (e[:-2] + e[2:])))

    for q in range(6):
        rows[q, pl.ds(0, 16, stride=2)] = e[q]
        rows[q, pl.ds(1, 16, stride=2)] = e[q]
    for copy in fifth:
        copy.wait_recv()
    e = jnp.stack([e1[l + 3] + rows[l // 2 + 2, pl.ds(0, 32)] for l in range(-3, 7)])
    for n in range(2):
        inner = slice(n, 8 - n)
        x = e[1:-1]
        e = (1.0 - OMEGA) * x + ws[inner] * (fs[inner] + k1 * (ring(x, 2) + (e[:-2] + e[2:])))
    for q in range(6):
        rows[q, pl.ds(0, 32, stride=2)] = e[q]
        rows[q, pl.ds(1, 32, stride=2)] = e[q]

    relay(2, 0)

    for copy in second:
        copy.wait_recv()

    def correct(q, carry):
        fields = split(rows[q], 1)
        for i in range(2):
            for h in range(2):
                ea[i, 2 * q + h] = eb[i, 2 * q + h] + fields[i]
        return carry

    lax.fori_loop(0, 6, correct, 0)
    for copy in second:
        copy.wait_send()

    def sweep_up(l, carry):
        for i in range(2):
            x = ea[i, l + 1]
            around = ring(x, 1) + (ea[i, l] + ea[i, l + 2])
            eb[i, l + 1] = (1.0 - OMEGA) * x + w[i, l] * (f[i, l] + KINETIC * around)
        return carry

    lax.fori_loop(0, layers + 2, sweep_up, 0)

    def sweep_last(l, carry):
        for i in range(2):
            x = eb[i, l + 2]
            around = ring(x, 1) + (eb[i, l + 1] + eb[i, l + 3])
            ea[i, l] = g[i, l + 1] + (
                (1.0 - OMEGA) * x + w[i, l + 1] * (f[i, l + 1] + KINETIC * around)
            )
        return carry

    lax.fori_loop(cut, layers, sweep_last, 0)

    @pl.when(is_outer)
    def _():
        visit.start()

    lax.fori_loop(0, cut, sweep_last, 0)

    def intersect(q, h, start, stop):
        def products(n, sums):
            l, r = lax.div(n, 8), pl.ds(pl.multiple_of(lax.rem(n, 8) * 8, 8), 8)
            u = [ea[i, l, r, :] for i in range(2)]
            new = []
            for c in range(2):
                x = orbs[2 * q + c, h, l, r, :]
                new += [sums[2 * c + i] + x * u[i] for i in range(2)]
            return tuple(new)

        sums = lax.fori_loop(start, stop, products, (jnp.zeros((8, 128), F32),) * 4, unroll=8)
        for m in range(4):
            row = pl.ds(4 * (m // 2) + 2 * h + m % 2, 1)
            found = jnp.sum(sums[m], axis=0, keepdims=True)
            gram[q, row, :] = found

    pair_side, odd = lax.div(chip, 2), lax.rem(chip, 2)
    ways = [
        (chip + 1 - 2 * odd, 1 - odd),
        (2 - pair_side, 1 - pair_side),
        (3 - 3 * pair_side, 1 - pair_side),
    ]
    for copy in own:
        copy.wait_recv()
    for h in range(2):
        intersect(chip, h, 0, 64)
    for n, (q, is_down) in enumerate(ways):
        away = (q - chip) * (2 * is_down - 1)
        slot_of = 12 + 6 * is_down + 2 * away
        block = 2 * q + 1 - core
        for h in range(2):
            if n == 1 and h == 1:
                relay(2, 1)
            if n < 2:
                hand(block, h, slot_of + h, mate).wait_recv()
                intersect(q, h, 0, 64)
                continue
            relay(3, h)

            @pl.when(is_outer)
            def _():
                hand(block, h, slot_of + h, mate, early).wait_recv()

            @pl.when(is_inner)
            def _():
                hand(block, h, slot_of + h, mate).wait_recv()
                intersect(q, h, 0, 64)

            @pl.when(is_outer)
            def _():
                intersect(q, h, 0, 8 * cut)

    @pl.when(is_inner)
    def _():
        visit.wait_recv()

        def products(n, sums):
            l, r = lax.div(n, 8), pl.ds(pl.multiple_of(lax.rem(n, 8) * 8, 8), 8)
            u = [guest[i, l, r, :] for i in range(2)]
            new = []
            for c in range(2):
                for h in range(2):
                    x = orbs[far - core + c, h, cut + l, r, :]
                    new += [sums[len(new) + i] + x * u[i] for i in range(2)]
            return tuple(new)

        sums = lax.fori_loop(0, 8 * LATE, products, (jnp.zeros((8, 128), F32),) * 8, unroll=4)
        for m in range(8):
            gram[4, pl.ds(m, 1), :] = jnp.sum(sums[m], axis=0, keepdims=True)
        answer.start()

    @pl.when(is_outer)
    def _():
        answer.wait_recv()
        last = 3 - 3 * lax.div(chip, 2)
        gram[last] = gram[last] + gram[5]

    diagonal = lax.broadcasted_iota(jnp.int32, (32, 128), 0) == lax.broadcasted_iota(
        jnp.int32, (32, 128), 1
    )

    def lay(column):
        return jnp.sum(jnp.where(diagonal, column, 0.0), axis=0, keepdims=True)

    part[0] = lay(jnp.sum(gram[pl.ds(0, 4)].reshape(32, 128), axis=1, keepdims=True))
    sixth = [
        to_dom(part.at[0], part.at[k], gram_send, gram_recv, k - 1, rest[k - 1])
        for k in range(1, doms)
    ]
    for copy in sixth:
        copy.start()

    @pl.when(chip == 2)
    def _():
        for copy in late_up:
            copy.start()

    @pl.when(chip == 1)
    def _():
        for copy in late_down:
            copy.start()

    for copy in sixth:
        copy.wait_recv()
    total = jnp.sum(part[...], axis=0) * (1.0 / cells)
    coef[...] = jnp.broadcast_to(
        jnp.sum(jnp.where(diagonal, total, 0.0), axis=1, keepdims=True), (32, 128)
    )
    factors = [jnp.broadcast_to(coef[pl.ds(m, 1), :], (8, 128)) for m in range(32)]

    def project(n, carry):
        l, r = lax.div(n, 8), pl.ds(pl.multiple_of(lax.rem(n, 8) * 8, 8), 8)
        lost = [None, None]
        for j in range(16):
            x = orbs[j // 2, j % 2, l, r, :]
            for i in range(2):
                term = factors[2 * j + i] * x
                lost[i] = term if lost[i] is None else lost[i] + term
        for i in range(2):
            eb[i, l, r, :] = ea[i, l, r, :] - lost[i]
        return carry

    for h in range(2):

        @pl.when(chip == 3)
        def _():
            hand(far, h, 26 + h, mate, late).wait_recv()

        @pl.when(chip == 0)
        def _():
            hand(far, h, 28 + h, mate, late).wait_recv()

    @pl.when(is_outer)
    def _():
        for copy in late_share:
            copy.start()

    stores = []
    bounds = [0, 2, cut, layers - 1, layers]
    for k in range(4):
        if k == 2:

            @pl.when(is_outer)
            def _():
                for h in range(2):
                    hand(far + 1 - 2 * core, h, 30 + h, mate, late).wait_recv()

        lax.fori_loop(8 * bounds[k], 8 * bounds[k + 1], project, 0, unroll=2)
        part_of = pl.ds(bounds[k], bounds[k + 1] - bounds[k])
        stores.append(pltpu.make_async_copy(eb.at[:, part_of], out.at[:, part_of], load_sem.at[k]))
        stores[k].start()

    for copy in first + static + swap + third + fourth + fifth + sixth:
        copy.wait_send()
    for copy in own:
        copy.wait_send()
    for h in range(2):
        for n in range(3):

            @pl.when((chip >= n) & (chip < 3))
            def _():
                up(n, h).wait_send()

            @pl.when((chip <= 3 - n) & (chip > 0))
            def _():
                down(n, h).wait_send()

        for n in range(1, 4):

            @pl.when(chip >= n)
            def _():
                share_up(n, h).wait_send()

            @pl.when(chip <= 3 - n)
            def _():
                share_down(n, h).wait_send()

    @pl.when(is_outer)
    def _():
        for copy in late_share + [visit]:
            copy.wait_send()

    @pl.when(is_inner)
    def _():
        answer.wait_send()

    @pl.when(chip == 2)
    def _():
        for copy in late_up:
            copy.wait_send()

    @pl.when(chip == 1)
    def _():
        for copy in late_down:
            copy.wait_send()

    for store in stores:
        store.wait()


def on_device(orbitals, initial_guess, potential, perturbation, level_shifts, assignment):
    doms = lax.axis_size("dom")
    cells = orbitals.shape[1] * doms * orbitals.shape[2] * orbitals.shape[3]
    dma = pltpu.SemaphoreType.DMA
    vmem = pltpu.VMEM

    def field(*shape):
        return vmem(shape, F32)

    anywhere = pl.BlockSpec(memory_space=pltpu.HBM)
    return pl.pallas_call(
        functools.partial(kernel, cells),
        out_shape=jax.ShapeDtypeStruct(orbitals.shape, F32),
        in_specs=[anywhere] * 6,
        out_specs=anywhere,
        scratch_shapes=[
            field(8, 2, 8, 64, 128),
            field(2, 10, 64, 128),
            field(8, 64, 128),
            field(8, 64, 128),
            field(2, 2, 64, 128),
            field(2, 96, 128),
            field(2, 96, 128),
            field(16, 128),
            field(6, 16, 128),
            field(2, 2, 2, 64, 128),
            field(2, 2, 2, 64, 128),
            field(2, 10, 64, 128),
            field(2, 10, 64, 128),
            field(2, 12, 64, 128),
            field(2, 12, 64, 128),
            field(8, 32, 128),
            field(8, 32, 128),
            field(8, 32, 128),
            field(10, 32, 128),
            field(16, 128),
            field(6, 16, 128),
            field(6, 64, 128),
            field(6, 8, 128),
            field(2, LATE, 64, 128),
            field(doms, 1, 128),
            field(32, 128),
            pltpu.SMEM((16,), F32),
            pltpu.SMEM((2,), jnp.int32),
            dma((6,)),
            dma((12,)),
            dma((12,)),
            dma((12,)),
            dma((12,)),
            dma((34,)),
            dma((34,)),
            dma((doms - 1,)),
            dma((doms - 1,)),
        ],
        compiler_params=pltpu.CompilerParams(
            collective_id=0, has_side_effects=True, vmem_limit_bytes=67043328
        ),
        name="sternheimer",
    )(orbitals, initial_guess, potential, perturbation, level_shifts, assignment)


def solution(mesh):
    in_specs = (
        P("orb", "dom", None, None),
        P("orb", "dom", None, None),
        P("dom", None, None),
        P("dom", None, None),
        P(),
        P("orb"),
    )
    out_specs = P("orb", "dom", None, None)
    return jax.shard_map(
        on_device, mesh=mesh, in_specs=in_specs, out_specs=out_specs, check_vma=False
    )
```

```python
import functools

import jax
import jax.numpy as jnp
from jax import lax
from jax.experimental import pallas as pl
from jax.experimental.pallas import tpu as pltpu
from jax.sharding import PartitionSpec as P

OMEGA = 0.8
LATE = 4
KINETIC = 8.0
MESH = pl.DeviceIdType.MESH
F32 = jnp.float32


def turn(x, shift, axis):
    return pltpu.roll(x, shift % x.shape[axis], axis)


def ring(x, step):
    ya, za = x.ndim - 2, x.ndim - 1
    return (turn(x, 1, ya) + turn(x, -1, ya)) + (turn(x, step, za) + turn(x, -step, za))


def lane_bit(shape, bit):
    return (lax.broadcasted_iota(jnp.int32, shape, len(shape) - 1) & bit) == 0


def pair(first, second, bit):
    za = first.ndim - 1
    return jnp.where(
        lane_bit(first.shape, bit), first + turn(first, -bit, za), second + turn(second, bit, za)
    )


def split(packed, bit):
    za = packed.ndim - 1
    clear = lane_bit(packed.shape, bit)
    return (
        jnp.where(clear, packed, turn(packed, bit, za)),
        jnp.where(clear, turn(packed, -bit, za), packed),
    )


def kernel(
    cells, orb_in, guess_in, pot_in, pert_in, table_in, slot_in, out,
    orbs, g, pot, pert, gh, st_out, st_in, c2_out, c2_in, fe_out, fe_in,
    f, w, ea, eb, f1, c1, w1, e1, f2_out, f2_in, rows, gram, guest, part, coef,
    table, slot, load_sem, halo_send, halo_recv, wide_send, wide_recv, ag_send, ag_recv,
    gram_send, gram_recv,
):
    d = lax.axis_index("dom")
    o = lax.axis_index("orb")
    doms = lax.axis_size("dom")
    layers, half, quarter = 8, 4, 2

    barrier = pltpu.get_barrier_semaphore()
    near = [lax.rem(d + doms + k, doms) for k in (-3, -2, -1, 1, 2, 3)]
    rest = [lax.rem(d + k, doms) for k in range(1, doms)]
    chip, core = lax.div(o, 2), lax.rem(o, 2)
    mate = o + 1 - 2 * core
    others = [mate] + [lax.rem(o + 2 * k, 8) for k in range(1, 4)]
    for there in rest:
        pl.semaphore_signal(barrier, inc=1, device_id={"dom": there}, device_id_type=MESH)
    for there in others:
        pl.semaphore_signal(barrier, inc=1, device_id={"orb": there}, device_id_type=MESH)

    loads = [
        pltpu.make_async_copy(guess_in, g.at[:, pl.ds(1, layers)], load_sem.at[0]),
        pltpu.make_async_copy(orb_in, orbs.at[o], load_sem.at[1]),
        pltpu.make_async_copy(pot_in, pot, load_sem.at[2]),
        pltpu.make_async_copy(pert_in, pert, load_sem.at[3]),
        pltpu.make_async_copy(table_in, table, load_sem.at[4]),
        pltpu.make_async_copy(slot_in, slot, load_sem.at[5]),
    ]
    for copy in loads:
        copy.start()
    zero = jnp.zeros((64, 128), F32)
    for i in range(2):
        g[i, 0] = zero
        g[i, layers + 1] = zero
    for copy in loads:
        copy.wait()
    shift = [table[slot[i]] for i in range(2)]
    base = [6.0 * KINETIC + s for s in shift]

    def start_layer(l, carry):
        p, q = pot[l], pert[l]
        for i in range(2):
            x = g[i, l + 1]
            diag = p + base[i]
            around = ring(x, 1) + (g[i, l] + g[i, l + 2])
            f[i, l + 1] = KINETIC * around - diag * x - q * orbs[o, i, l]
            w[i, l + 1] = OMEGA / diag
        return carry

    lax.fori_loop(0, layers, start_layer, 0, unroll=2)
    for side, (edge, inner) in enumerate(((1, 2), (layers, layers - 1))):
        for i in range(2):
            fe_out[side, 0, i] = f[i, edge]
            fe_out[side, 1, i] = w[i, inner] * f[i, inner]

    for q in range(half):
        t = pot[2 * q] + pot[2 * q + 1]
        rows[q] = pair(t, t, 1)
    for q in range(half):
        c1[q + 2] = 0.125 * (rows[q, pl.ds(0, 32, stride=2)] + rows[q, pl.ds(1, 32, stride=2)])
    even = lane_bit((32, 128), 1)
    st_out[0, pl.ds(0, 64)] = pot[0]
    st_out[1, pl.ds(0, 64)] = pot[layers - 1]
    st_out[0, pl.ds(64, 32)] = jnp.where(even, c1[2], c1[3])
    st_out[1, pl.ds(64, 32)] = jnp.where(even, c1[4], c1[5])
    for q in range(quarter):
        t = c1[2 * q + 2] + c1[2 * q + 3]
        rows[q, pl.ds(0, 32)] = pair(t, t, 2)
    c2 = [
        0.125 * (rows[q, pl.ds(0, 16, stride=2)] + rows[q, pl.ds(1, 16, stride=2)])
        for q in range(quarter)
    ]
    low = lane_bit((16, 128), 2)
    c2_out[...] = jnp.where(low, c2[0], c2[1])

    pl.semaphore_wait(barrier, len(rest) + len(others))

    def to_dom(src, dst, sends, recvs, k, there):
        return pltpu.make_async_remote_copy(
            src_ref=src, dst_ref=dst, send_sem=sends.at[k], recv_sem=recvs.at[k],
            device_id={"dom": there}, device_id_type=MESH,
        )

    below, above = near[2], near[3]
    first = []
    for side, there in ((0, below), (1, above)):
        edge = 1 if side == 0 else layers
        first += [
            to_dom(fe_out.at[side], fe_in.at[1 - side], halo_send, halo_recv, side, there),
            to_dom(g.at[:, edge], gh.at[1 - side], halo_send, halo_recv, 2 + side, there),
        ]
    ahead = 1 - 2 * core
    static = [
        to_dom(
            st_out.at[1 - core], st_in.at[core], halo_send, halo_recv, 4,
            lax.rem(d + doms + ahead, doms),
        )
    ]
    for n in range(1, 4):
        place = core * (2 + n) + (1 - core) * (3 - n)
        static.append(
            to_dom(
                c2_out, c2_in.at[place], wide_send, wide_recv, n,
                lax.rem(d + doms + n * ahead, doms),
            )
        )
    for copy in static[:1] + first + static[1:]:
        copy.start()

    cut = layers - LATE
    early, late = pl.ds(0, cut), pl.ds(cut, LATE)
    is_inner = (chip == 1) | (chip == 2)
    is_outer = (chip == 0) | (chip == 3)

    def hand(block, h, k, there, part=pl.ds(0, 8)):
        return pltpu.make_async_remote_copy(
            src_ref=orbs.at[block, h, part], dst_ref=orbs.at[block, h, part],
            send_sem=ag_send.at[k], recv_sem=ag_recv.at[k],
            device_id={"orb": there}, device_id_type=MESH,
        )

    def reach(n, most):
        return early if n == most else pl.ds(0, 8)

    def up(n, h):
        return hand(o - 2 * n, h, 2 * n + h, o + 2, reach(n, 2))

    def down(n, h):
        return hand(o + 2 * n, h, 6 + 2 * n + h, o - 2, reach(n, 2))

    def share_up(n, h):
        return hand(o - 2 * n, h, 12 + 2 * n + h, mate, reach(n, 3))

    def share_down(n, h):
        return hand(o + 2 * n, h, 18 + 2 * n + h, mate, reach(n, 3))

    late_up = [hand(o - 4, h, 26 + h, o + 2, late) for h in range(2)]
    late_down = [hand(o + 4, h, 28 + h, o - 2, late) for h in range(2)]
    near_end = o + 2 - 4 * lax.rem(chip, 2)
    far = 2 * (3 - 3 * lax.div(chip, 2)) + core
    late_share = [hand(far, h, 30 + h, mate, late) for h in range(2)]
    visit = pltpu.make_async_remote_copy(
        src_ref=ea.at[:, late], dst_ref=guest,
        send_sem=ag_send.at[32], recv_sem=ag_recv.at[32],
        device_id={"orb": near_end}, device_id_type=MESH,
    )
    answer = pltpu.make_async_remote_copy(
        src_ref=gram.at[4], dst_ref=gram.at[5],
        send_sem=ag_send.at[33], recv_sem=ag_recv.at[33],
        device_id={"orb": near_end}, device_id_type=MESH,
    )
    own = [hand(o, h, 12 + h, mate) for h in range(2)]

    def relay(n, h):
        @pl.when(chip >= n)
        def _():
            hand(o - 2 * n, h, 2 * (n - 1) + h, mate, reach(n, 3)).wait_recv()
            if n < 3:

                @pl.when(chip < 3)
                def _():
                    up(n, h).start()

            share_up(n, h).start()

        @pl.when(chip <= 3 - n)
        def _():
            hand(o + 2 * n, h, 6 + 2 * (n - 1) + h, mate, reach(n, 3)).wait_recv()
            if n < 3:

                @pl.when(chip > 0)
                def _():
                    down(n, h).start()

            share_down(n, h).start()

    for h in range(2):

        @pl.when(chip < 3)
        def _():
            up(0, h).start()

        @pl.when(chip > 0)
        def _():
            down(0, h).start()

    for copy in own:
        copy.start()

    static[0].wait_recv()
    swap = [
        pltpu.make_async_remote_copy(
            src_ref=st_in.at[core], dst_ref=st_in.at[core],
            send_sem=halo_send.at[5], recv_sem=halo_recv.at[5],
            device_id={"orb": mate}, device_id_type=MESH,
        )
    ]
    swap[0].start()
    for copy in first:
        copy.wait_recv()

    swap[0].wait_recv()

    for i in range(2):
        f[i, 1] = f[i, 1] + KINETIC * gh[0, i]
        f[i, layers] = f[i, layers] + KINETIC * gh[1, i]
        for side, (beyond, edge, rim) in enumerate(((0, 1, 0), (layers + 1, layers, 11))):
            f[i, beyond] = fe_in[side, 0, i] + KINETIC * g[i, edge]
            w[i, beyond] = OMEGA / (st_in[side, pl.ds(0, 64)] + base[i])
            ea[i, rim] = fe_in[side, 1, i]
    c1[0], c1[1] = split(st_in[0, pl.ds(64, 32)], 1)
    c1[6], c1[7] = split(st_in[1, pl.ds(64, 32)], 1)

    def begin(l, carry):
        for i in range(2):
            ea[i, l + 1] = w[i, l] * f[i, l]
        return carry

    lax.fori_loop(0, layers + 2, begin, 0, unroll=2)

    def sweep_down(l, carry):
        for i in range(2):
            around = ring(ea[i, l + 1], 1) + (ea[i, l] + ea[i, l + 2])
            eb[i, l + 1] = w[i, l] * ((2.0 - OMEGA) * f[i, l] + KINETIC * around)
        return carry

    lax.fori_loop(0, layers + 2, sweep_down, 0, unroll=2)
    second = [
        to_dom(eb.at[:, 3], eb.at[:, 11], halo_send, halo_recv, 6, below),
        to_dom(eb.at[:, 8], eb.at[:, 0], halo_send, halo_recv, 7, above),
    ]

    def remainder(q, carry):
        total = []
        for i in range(2):
            parts = []
            for h in range(2):
                l = 2 * q + h
                x = eb[i, l + 2]
                around = ring(x, 1) + (eb[i, l + 1] + eb[i, l + 3])
                parts.append(f[i, l + 1] + KINETIC * around - (pot[l] + base[i]) * x)
            total.append(parts[0] + parts[1])
        rows[q] = pair(total[0], total[1], 1)
        return carry

    lax.fori_loop(0, half, remainder, 0, unroll=2)
    for q in range(half):
        f1[q + 2] = 0.125 * (rows[q, pl.ds(0, 32, stride=2)] + rows[q, pl.ds(1, 32, stride=2)])
    third = [
        to_dom(f1.at[pl.ds(2, 2)], f1.at[pl.ds(6, 2)], halo_send, halo_recv, 8, below),
        to_dom(f1.at[pl.ds(4, 2)], f1.at[pl.ds(0, 2)], halo_send, halo_recv, 9, above),
    ]
    for copy in third + second:
        copy.start()
    for copy in static[1:]:
        copy.wait_recv()
    swap.append(
        pltpu.make_async_remote_copy(
            src_ref=c2_in.at[pl.ds(3 * core, 3)], dst_ref=c2_in.at[pl.ds(3 * core, 3)],
            send_sem=wide_send.at[0], recv_sem=wide_recv.at[0],
            device_id={"orb": mate}, device_id_type=MESH,
        )
    )
    swap[1].start()

    k1, k2 = KINETIC / 4, KINETIC / 16
    both = jnp.where(even, shift[0], shift[1])
    for q in range(8):
        w1[q] = OMEGA / (c1[q] + (6.0 * k1 + both))
    swap[1].wait_recv()
    both2 = jnp.where(lane_bit((16, 128), 1), shift[0], shift[1])
    c2s = []
    for k in range(3):
        c2s += split(c2_in[k], 2)
    c2s += c2
    for k in range(3, 6):
        c2s += split(c2_in[k], 2)
    w2 = jnp.stack([OMEGA / (c + (6.0 * k2 + both2)) for c in c2s[1:13]])

    for copy in third:
        copy.wait_recv()
    fs, ws = f1[...], w1[...]
    e = ws * fs
    e = ws[1:7] * ((2.0 - OMEGA) * fs[1:7] + k1 * (ring(e[1:7], 2) + (e[:6] + e[2:])))
    e1[pl.ds(2, 6)] = e
    x = e[1:5]
    r = fs[2:6] + k1 * (ring(x, 2) + (e[:4] + e[2:])) - (c1[pl.ds(2, 4)] + (6.0 * k1 + both)) * x
    for q in range(quarter):
        t = r[2 * q] + r[2 * q + 1]
        rows[q, pl.ds(0, 32)] = pair(t, t, 2)
    f2 = [
        0.125 * (rows[q, pl.ds(0, 16, stride=2)] + rows[q, pl.ds(1, 16, stride=2)])
        for q in range(quarter)
    ]
    f2_out[...] = jnp.where(low, f2[0], f2[1])
    fourth = [
        to_dom(f2_out, f2_in.at[5 - k], wide_send, wide_recv, 6 + k, near[k]) for k in range(6)
    ]
    fifth = [
        to_dom(e1.at[pl.ds(4, 2)], e1.at[pl.ds(8, 2)], halo_send, halo_recv, 10, below),
        to_dom(e1.at[pl.ds(4, 2)], e1.at[pl.ds(0, 2)], halo_send, halo_recv, 11, above),
    ]
    for copy in fourth + fifth:
        copy.start()
    relay(1, 0)
    relay(1, 1)
    for copy in fourth:
        copy.wait_recv()

    f2s = []
    for k in range(3):
        f2s += split(f2_in[k], 2)
    f2s += f2
    for k in range(3, 6):
        f2s += split(f2_in[k], 2)
    f2v = jnp.stack(f2s[1:13])
    e = w2 * f2v
    for n in range(1, 4):
        inner = slice(n, 12 - n)
        x = e[1:-1]
        e = (1.0 - OMEGA) * x + w2[inner] * (f2v[inner] + k2 * (ring(x, 4) + (e[:-2] + e[2:])))

    for q in range(6):
        rows[q, pl.ds(0, 16, stride=2)] = e[q]
        rows[q, pl.ds(1, 16, stride=2)] = e[q]
    for copy in fifth:
        copy.wait_recv()
    e = jnp.stack([e1[l + 3] + rows[l // 2 + 2, pl.ds(0, 32)] for l in range(-3, 7)])
    for n in range(2):
        inner = slice(n, 8 - n)
        x = e[1:-1]
        e = (1.0 - OMEGA) * x + ws[inner] * (fs[inner] + k1 * (ring(x, 2) + (e[:-2] + e[2:])))
    for q in range(6):
        rows[q, pl.ds(0, 32, stride=2)] = e[q]
        rows[q, pl.ds(1, 32, stride=2)] = e[q]

    relay(2, 0)

    for copy in second:
        copy.wait_recv()

    def correct(q, carry):
        fields = split(rows[q], 1)
        for i in range(2):
            for h in range(2):
                ea[i, 2 * q + h] = eb[i, 2 * q + h] + fields[i]
        return carry

    lax.fori_loop(0, 6, correct, 0, unroll=2)
    for copy in second:
        copy.wait_send()

    def sweep_up(l, carry):
        for i in range(2):
            x = ea[i, l + 1]
            around = ring(x, 1) + (ea[i, l] + ea[i, l + 2])
            eb[i, l + 1] = (1.0 - OMEGA) * x + w[i, l] * (f[i, l] + KINETIC * around)
        return carry

    lax.fori_loop(0, layers + 2, sweep_up, 0, unroll=2)

    def sweep_last(l, carry):
        for i in range(2):
            x = eb[i, l + 2]
            around = ring(x, 1) + (eb[i, l + 1] + eb[i, l + 3])
            ea[i, l] = g[i, l + 1] + (
                (1.0 - OMEGA) * x + w[i, l + 1] * (f[i, l + 1] + KINETIC * around)
            )
        return carry

    lax.fori_loop(cut, layers, sweep_last, 0, unroll=2)

    @pl.when(is_outer)
    def _():
        visit.start()

    lax.fori_loop(0, cut, sweep_last, 0, unroll=2)

    def intersect(q, h, start, stop):
        def products(n, sums):
            l, r = lax.div(n, 8), pl.ds(pl.multiple_of(lax.rem(n, 8) * 8, 8), 8)
            u = [ea[i, l, r, :] for i in range(2)]
            new = []
            for c in range(2):
                x = orbs[2 * q + c, h, l, r, :]
                new += [sums[2 * c + i] + x * u[i] for i in range(2)]
            return tuple(new)

        sums = lax.fori_loop(start, stop, products, (jnp.zeros((8, 128), F32),) * 4, unroll=8)
        for m in range(4):
            row = pl.ds(4 * (m // 2) + 2 * h + m % 2, 1)
            found = jnp.sum(sums[m], axis=0, keepdims=True)
            gram[q, row, :] = found

    pair_side, odd = lax.div(chip, 2), lax.rem(chip, 2)
    ways = [
        (chip + 1 - 2 * odd, 1 - odd),
        (2 - pair_side, 1 - pair_side),
        (3 - 3 * pair_side, 1 - pair_side),
    ]
    for copy in own:
        copy.wait_recv()
    for h in range(2):
        intersect(chip, h, 0, 64)
    for n, (q, is_down) in enumerate(ways):
        away = (q - chip) * (2 * is_down - 1)
        slot_of = 12 + 6 * is_down + 2 * away
        block = 2 * q + 1 - core
        for h in range(2):
            if n == 1 and h == 1:
                relay(2, 1)
            if n < 2:
                hand(block, h, slot_of + h, mate).wait_recv()
                intersect(q, h, 0, 64)
                continue
            relay(3, h)

            @pl.when(is_outer)
            def _():
                hand(block, h, slot_of + h, mate, early).wait_recv()

            @pl.when(is_inner)
            def _():
                hand(block, h, slot_of + h, mate).wait_recv()
                intersect(q, h, 0, 64)

            @pl.when(is_outer)
            def _():
                intersect(q, h, 0, 8 * cut)

    @pl.when(is_inner)
    def _():
        visit.wait_recv()

        def products(n, sums):
            l, r = lax.div(n, 8), pl.ds(pl.multiple_of(lax.rem(n, 8) * 8, 8), 8)
            u = [guest[i, l, r, :] for i in range(2)]
            new = []
            for c in range(2):
                for h in range(2):
                    x = orbs[far - core + c, h, cut + l, r, :]
                    new += [sums[len(new) + i] + x * u[i] for i in range(2)]
            return tuple(new)

        sums = lax.fori_loop(0, 8 * LATE, products, (jnp.zeros((8, 128), F32),) * 8, unroll=4)
        for m in range(8):
            gram[4, pl.ds(m, 1), :] = jnp.sum(sums[m], axis=0, keepdims=True)
        answer.start()

    @pl.when(is_outer)
    def _():
        answer.wait_recv()
        last = 3 - 3 * lax.div(chip, 2)
        gram[last] = gram[last] + gram[5]

    diagonal = lax.broadcasted_iota(jnp.int32, (32, 128), 0) == lax.broadcasted_iota(
        jnp.int32, (32, 128), 1
    )

    def lay(column):
        return jnp.sum(jnp.where(diagonal, column, 0.0), axis=0, keepdims=True)

    part[0] = lay(jnp.sum(gram[pl.ds(0, 4)].reshape(32, 128), axis=1, keepdims=True))
    sixth = [
        to_dom(part.at[0], part.at[k], gram_send, gram_recv, k - 1, rest[k - 1])
        for k in range(1, doms)
    ]
    for copy in sixth:
        copy.start()

    @pl.when(chip == 2)
    def _():
        for copy in late_up:
            copy.start()

    @pl.when(chip == 1)
    def _():
        for copy in late_down:
            copy.start()

    for h in range(2):

        @pl.when(chip == 3)
        def _():
            hand(far, h, 26 + h, mate, late).wait_recv()
            late_share[h].start()

        @pl.when(chip == 0)
        def _():
            hand(far, h, 28 + h, mate, late).wait_recv()
            late_share[h].start()

    for copy in sixth:
        copy.wait_recv()
    total = jnp.sum(part[...], axis=0) * (1.0 / cells)
    coef[...] = jnp.broadcast_to(
        jnp.sum(jnp.where(diagonal, total, 0.0), axis=1, keepdims=True), (32, 128)
    )
    factors = [jnp.broadcast_to(coef[pl.ds(m, 1), :], (8, 128)) for m in range(32)]

    def project(n, carry):
        l, r = lax.div(n, 8), pl.ds(pl.multiple_of(lax.rem(n, 8) * 8, 8), 8)
        lost = [None, None]
        for j in range(16):
            x = orbs[j // 2, j % 2, l, r, :]
            for i in range(2):
                term = factors[2 * j + i] * x
                lost[i] = term if lost[i] is None else lost[i] + term
        for i in range(2):
            eb[i, l, r, :] = ea[i, l, r, :] - lost[i]
        return carry

    stores = []
    bounds = [0, 2, cut, layers - 1, layers]
    for k in range(4):
        if k == 2:

            @pl.when(is_outer)
            def _():
                for h in range(2):
                    hand(far + 1 - 2 * core, h, 30 + h, mate, late).wait_recv()

        lax.fori_loop(8 * bounds[k], 8 * bounds[k + 1], project, 0, unroll=2)
        part_of = pl.ds(bounds[k], bounds[k + 1] - bounds[k])
        stores.append(pltpu.make_async_copy(eb.at[:, part_of], out.at[:, part_of], load_sem.at[k]))
        stores[k].start()

    for copy in first + static + swap + third + fourth + fifth + sixth:
        copy.wait_send()
    for copy in own:
        copy.wait_send()
    for h in range(2):
        for n in range(3):

            @pl.when((chip >= n) & (chip < 3))
            def _():
                up(n, h).wait_send()

            @pl.when((chip <= 3 - n) & (chip > 0))
            def _():
                down(n, h).wait_send()

        for n in range(1, 4):

            @pl.when(chip >= n)
            def _():
                share_up(n, h).wait_send()

            @pl.when(chip <= 3 - n)
            def _():
                share_down(n, h).wait_send()

    @pl.when(is_outer)
    def _():
        for copy in late_share + [visit]:
            copy.wait_send()

    @pl.when(is_inner)
    def _():
        answer.wait_send()

    @pl.when(chip == 2)
    def _():
        for copy in late_up:
            copy.wait_send()

    @pl.when(chip == 1)
    def _():
        for copy in late_down:
            copy.wait_send()

    for store in stores:
        store.wait()


def on_device(orbitals, initial_guess, potential, perturbation, level_shifts, assignment):
    doms = lax.axis_size("dom")
    cells = orbitals.shape[1] * doms * orbitals.shape[2] * orbitals.shape[3]
    dma = pltpu.SemaphoreType.DMA
    vmem = pltpu.VMEM

    def field(*shape):
        return vmem(shape, F32)

    anywhere = pl.BlockSpec(memory_space=pltpu.HBM)
    return pl.pallas_call(
        functools.partial(kernel, cells),
        out_shape=jax.ShapeDtypeStruct(orbitals.shape, F32),
        in_specs=[anywhere] * 6,
        out_specs=anywhere,
        scratch_shapes=[
            field(8, 2, 8, 64, 128),
            field(2, 10, 64, 128),
            field(8, 64, 128),
            field(8, 64, 128),
            field(2, 2, 64, 128),
            field(2, 96, 128),
            field(2, 96, 128),
            field(16, 128),
            field(6, 16, 128),
            field(2, 2, 2, 64, 128),
            field(2, 2, 2, 64, 128),
            field(2, 10, 64, 128),
            field(2, 10, 64, 128),
            field(2, 12, 64, 128),
            field(2, 12, 64, 128),
            field(8, 32, 128),
            field(8, 32, 128),
            field(8, 32, 128),
            field(10, 32, 128),
            field(16, 128),
            field(6, 16, 128),
            field(6, 64, 128),
            field(6, 8, 128),
            field(2, LATE, 64, 128),
            field(doms, 1, 128),
            field(32, 128),
            pltpu.SMEM((16,), F32),
            pltpu.SMEM((2,), jnp.int32),
            dma((6,)),
            dma((12,)),
            dma((12,)),
            dma((12,)),
            dma((12,)),
            dma((34,)),
            dma((34,)),
            dma((doms - 1,)),
            dma((doms - 1,)),
        ],
        compiler_params=pltpu.CompilerParams(
            collective_id=0, has_side_effects=True, vmem_limit_bytes=67043328
        ),
        name="sternheimer",
    )(orbitals, initial_guess, potential, perturbation, level_shifts, assignment)


def solution(mesh):
    in_specs = (
        P("orb", "dom", None, None),
        P("orb", "dom", None, None),
        P("dom", None, None),
        P("dom", None, None),
        P(),
        P("orb"),
    )
    out_specs = P("orb", "dom", None, None)
    return jax.shard_map(
        on_device, mesh=mesh, in_specs=in_specs, out_specs=out_specs, check_vma=False
    )
```

```python
import functools

import jax
import jax.numpy as jnp
from jax import lax
from jax.experimental import pallas as pl
from jax.experimental.pallas import tpu as pltpu
from jax.sharding import PartitionSpec as P

OMEGA = 0.8
LATE = 4
KINETIC = 8.0
MESH = pl.DeviceIdType.MESH
F32 = jnp.float32


def turn(x, shift, axis):
    return pltpu.roll(x, shift % x.shape[axis], axis)


def ring(x, step):
    ya, za = x.ndim - 2, x.ndim - 1
    return (turn(x, 1, ya) + turn(x, -1, ya)) + (turn(x, step, za) + turn(x, -step, za))


def lane_bit(shape, bit):
    return (lax.broadcasted_iota(jnp.int32, shape, len(shape) - 1) & bit) == 0


def pair(first, second, bit):
    za = first.ndim - 1
    return jnp.where(
        lane_bit(first.shape, bit), first + turn(first, -bit, za), second + turn(second, bit, za)
    )


def split(packed, bit):
    za = packed.ndim - 1
    clear = lane_bit(packed.shape, bit)
    return (
        jnp.where(clear, packed, turn(packed, bit, za)),
        jnp.where(clear, turn(packed, -bit, za), packed),
    )


def kernel(
    cells, orb_in, guess_in, pot_in, pert_in, table_in, slot_in, out,
    orbs, g, pot, pert, gh, st_out, st_in, c2_out, c2_in, fe_out, fe_in,
    f, w, ea, eb, f1, c1, w1, e1, f2_out, f2_in, rows, gram, guest, part, coef,
    table, slot, load_sem, halo_send, halo_recv, wide_send, wide_recv, ag_send, ag_recv,
    gram_send, gram_recv,
):
    d = lax.axis_index("dom")
    o = lax.axis_index("orb")
    doms = lax.axis_size("dom")
    layers, half, quarter = 8, 4, 2

    barrier = pltpu.get_barrier_semaphore()
    near = [lax.rem(d + doms + k, doms) for k in (-3, -2, -1, 1, 2, 3)]
    rest = [lax.rem(d + k, doms) for k in range(1, doms)]
    chip, core = lax.div(o, 2), lax.rem(o, 2)
    mate = o + 1 - 2 * core
    others = [mate] + [lax.rem(o + 2 * k, 8) for k in range(1, 4)]
    for there in rest:
        pl.semaphore_signal(barrier, inc=1, device_id={"dom": there}, device_id_type=MESH)
    for there in others:
        pl.semaphore_signal(barrier, inc=1, device_id={"orb": there}, device_id_type=MESH)

    loads = [
        pltpu.make_async_copy(guess_in, g.at[:, pl.ds(1, layers)], load_sem.at[0]),
        pltpu.make_async_copy(orb_in, orbs.at[o], load_sem.at[1]),
        pltpu.make_async_copy(pot_in, pot, load_sem.at[2]),
        pltpu.make_async_copy(pert_in, pert, load_sem.at[3]),
        pltpu.make_async_copy(table_in, table, load_sem.at[4]),
        pltpu.make_async_copy(slot_in, slot, load_sem.at[5]),
    ]
    for copy in loads:
        copy.start()
    zero = jnp.zeros((64, 128), F32)
    for i in range(2):
        g[i, 0] = zero
        g[i, layers + 1] = zero
    for copy in loads:
        copy.wait()
    shift = [table[slot[i]] for i in range(2)]
    base = [6.0 * KINETIC + s for s in shift]

    def start_layer(l, carry):
        p, q = pot[l], pert[l]
        for i in range(2):
            x = g[i, l + 1]
            diag = p + base[i]
            around = ring(x, 1) + (g[i, l] + g[i, l + 2])
            f[i, l + 1] = KINETIC * around - diag * x - q * orbs[o, i, l]
            w[i, l + 1] = OMEGA / diag
        return carry

    lax.fori_loop(0, layers, start_layer, 0, unroll=2)
    for side, (edge, inner) in enumerate(((1, 2), (layers, layers - 1))):
        for i in range(2):
            fe_out[side, 0, i] = f[i, edge]
            fe_out[side, 1, i] = w[i, inner] * f[i, inner]

    for q in range(half):
        t = pot[2 * q] + pot[2 * q + 1]
        rows[q] = pair(t, t, 1)
    for q in range(half):
        c1[q + 2] = 0.125 * (rows[q, pl.ds(0, 32, stride=2)] + rows[q, pl.ds(1, 32, stride=2)])
    even = lane_bit((32, 128), 1)
    st_out[0, pl.ds(0, 64)] = pot[0]
    st_out[1, pl.ds(0, 64)] = pot[layers - 1]
    st_out[0, pl.ds(64, 32)] = jnp.where(even, c1[2], c1[3])
    st_out[1, pl.ds(64, 32)] = jnp.where(even, c1[4], c1[5])
    for q in range(quarter):
        t = c1[2 * q + 2] + c1[2 * q + 3]
        rows[q, pl.ds(0, 32)] = pair(t, t, 2)
    c2 = [
        0.125 * (rows[q, pl.ds(0, 16, stride=2)] + rows[q, pl.ds(1, 16, stride=2)])
        for q in range(quarter)
    ]
    low = lane_bit((16, 128), 2)
    c2_out[...] = jnp.where(low, c2[0], c2[1])

    pl.semaphore_wait(barrier, len(rest) + len(others))

    def to_dom(src, dst, sends, recvs, k, there):
        return pltpu.make_async_remote_copy(
            src_ref=src, dst_ref=dst, send_sem=sends.at[k], recv_sem=recvs.at[k],
            device_id={"dom": there}, device_id_type=MESH,
        )

    below, above = near[2], near[3]
    first = []
    for side, there in ((0, below), (1, above)):
        edge = 1 if side == 0 else layers
        first += [
            to_dom(fe_out.at[side], fe_in.at[1 - side], halo_send, halo_recv, side, there),
            to_dom(g.at[:, edge], gh.at[1 - side], halo_send, halo_recv, 2 + side, there),
        ]
    ahead = 1 - 2 * core
    static = [
        to_dom(
            st_out.at[1 - core], st_in.at[core], halo_send, halo_recv, 4,
            lax.rem(d + doms + ahead, doms),
        )
    ]
    for n in range(1, 4):
        place = core * (2 + n) + (1 - core) * (3 - n)
        static.append(
            to_dom(
                c2_out, c2_in.at[place], wide_send, wide_recv, n,
                lax.rem(d + doms + n * ahead, doms),
            )
        )
    for copy in static[:1] + first + static[1:]:
        copy.start()

    cut = layers - LATE
    early, late = pl.ds(0, cut), pl.ds(cut, LATE)
    is_inner = (chip == 1) | (chip == 2)
    is_outer = (chip == 0) | (chip == 3)

    def hand(block, h, k, there, part=pl.ds(0, 8)):
        return pltpu.make_async_remote_copy(
            src_ref=orbs.at[block, h, part], dst_ref=orbs.at[block, h, part],
            send_sem=ag_send.at[k], recv_sem=ag_recv.at[k],
            device_id={"orb": there}, device_id_type=MESH,
        )

    def reach(n, most):
        return early if n == most else pl.ds(0, 8)

    def up(n, h):
        return hand(o - 2 * n, h, 2 * n + h, o + 2, reach(n, 2))

    def down(n, h):
        return hand(o + 2 * n, h, 6 + 2 * n + h, o - 2, reach(n, 2))

    def share_up(n, h):
        return hand(o - 2 * n, h, 12 + 2 * n + h, mate, reach(n, 3))

    def share_down(n, h):
        return hand(o + 2 * n, h, 18 + 2 * n + h, mate, reach(n, 3))

    late_up = [hand(o - 4, h, 26 + h, o + 2, late) for h in range(2)]
    late_down = [hand(o + 4, h, 28 + h, o - 2, late) for h in range(2)]
    near_end = o + 2 - 4 * lax.rem(chip, 2)
    far = 2 * (3 - 3 * lax.div(chip, 2)) + core
    late_share = [hand(far, h, 30 + h, mate, late) for h in range(2)]
    visit = pltpu.make_async_remote_copy(
        src_ref=ea.at[:, late], dst_ref=guest,
        send_sem=ag_send.at[32], recv_sem=ag_recv.at[32],
        device_id={"orb": near_end}, device_id_type=MESH,
    )
    answer = pltpu.make_async_remote_copy(
        src_ref=gram.at[4], dst_ref=gram.at[5],
        send_sem=ag_send.at[33], recv_sem=ag_recv.at[33],
        device_id={"orb": near_end}, device_id_type=MESH,
    )
    own = [hand(o, h, 12 + h, mate) for h in range(2)]

    def relay(n, h):
        @pl.when(chip >= n)
        def _():
            hand(o - 2 * n, h, 2 * (n - 1) + h, mate, reach(n, 3)).wait_recv()
            if n < 3:

                @pl.when(chip < 3)
                def _():
                    up(n, h).start()

            share_up(n, h).start()

        @pl.when(chip <= 3 - n)
        def _():
            hand(o + 2 * n, h, 6 + 2 * (n - 1) + h, mate, reach(n, 3)).wait_recv()
            if n < 3:

                @pl.when(chip > 0)
                def _():
                    down(n, h).start()

            share_down(n, h).start()

    for h in range(2):

        @pl.when(chip < 3)
        def _():
            up(0, h).start()

        @pl.when(chip > 0)
        def _():
            down(0, h).start()

    static[0].wait_recv()
    swap = [
        pltpu.make_async_remote_copy(
            src_ref=st_in.at[core], dst_ref=st_in.at[core],
            send_sem=halo_send.at[5], recv_sem=halo_recv.at[5],
            device_id={"orb": mate}, device_id_type=MESH,
        )
    ]
    swap[0].start()
    for copy in first:
        copy.wait_recv()

    swap[0].wait_recv()

    for copy in own:
        copy.start()

    for i in range(2):
        f[i, 1] = f[i, 1] + KINETIC * gh[0, i]
        f[i, layers] = f[i, layers] + KINETIC * gh[1, i]
        for side, (beyond, edge, rim) in enumerate(((0, 1, 0), (layers + 1, layers, 11))):
            f[i, beyond] = fe_in[side, 0, i] + KINETIC * g[i, edge]
            w[i, beyond] = OMEGA / (st_in[side, pl.ds(0, 64)] + base[i])
            ea[i, rim] = fe_in[side, 1, i]
    c1[0], c1[1] = split(st_in[0, pl.ds(64, 32)], 1)
    c1[6], c1[7] = split(st_in[1, pl.ds(64, 32)], 1)

    def begin(l, carry):
        for i in range(2):
            ea[i, l + 1] = w[i, l] * f[i, l]
        return carry

    lax.fori_loop(0, layers + 2, begin, 0, unroll=2)

    def sweep_down(l, carry):
        for i in range(2):
            around = ring(ea[i, l + 1], 1) + (ea[i, l] + ea[i, l + 2])
            eb[i, l + 1] = w[i, l] * ((2.0 - OMEGA) * f[i, l] + KINETIC * around)
        return carry

    lax.fori_loop(0, layers + 2, sweep_down, 0, unroll=2)
    second = [
        to_dom(eb.at[:, 3], eb.at[:, 11], halo_send, halo_recv, 6, below),
        to_dom(eb.at[:, 8], eb.at[:, 0], halo_send, halo_recv, 7, above),
    ]

    def remainder(q, carry):
        total = []
        for i in range(2):
            parts = []
            for h in range(2):
                l = 2 * q + h
                x = eb[i, l + 2]
                around = ring(x, 1) + (eb[i, l + 1] + eb[i, l + 3])
                parts.append(f[i, l + 1] + KINETIC * around - (pot[l] + base[i]) * x)
            total.append(parts[0] + parts[1])
        rows[q] = pair(total[0], total[1], 1)
        return carry

    lax.fori_loop(0, half, remainder, 0, unroll=2)
    for q in range(half):
        f1[q + 2] = 0.125 * (rows[q, pl.ds(0, 32, stride=2)] + rows[q, pl.ds(1, 32, stride=2)])
    third = [
        to_dom(f1.at[pl.ds(2, 2)], f1.at[pl.ds(6, 2)], halo_send, halo_recv, 8, below),
        to_dom(f1.at[pl.ds(4, 2)], f1.at[pl.ds(0, 2)], halo_send, halo_recv, 9, above),
    ]
    for copy in third + second:
        copy.start()
    for copy in static[1:]:
        copy.wait_recv()
    swap.append(
        pltpu.make_async_remote_copy(
            src_ref=c2_in.at[pl.ds(3 * core, 3)], dst_ref=c2_in.at[pl.ds(3 * core, 3)],
            send_sem=wide_send.at[0], recv_sem=wide_recv.at[0],
            device_id={"orb": mate}, device_id_type=MESH,
        )
    )
    swap[1].start()

    k1, k2 = KINETIC / 4, KINETIC / 16
    both = jnp.where(even, shift[0], shift[1])
    for q in range(8):
        w1[q] = OMEGA / (c1[q] + (6.0 * k1 + both))
    swap[1].wait_recv()
    both2 = jnp.where(lane_bit((16, 128), 1), shift[0], shift[1])
    c2s = []
    for k in range(3):
        c2s += split(c2_in[k], 2)
    c2s += c2
    for k in range(3, 6):
        c2s += split(c2_in[k], 2)
    w2 = jnp.stack([OMEGA / (c + (6.0 * k2 + both2)) for c in c2s[1:13]])

    for copy in third:
        copy.wait_recv()
    fs, ws = f1[...], w1[...]
    e = ws * fs
    e = ws[1:7] * ((2.0 - OMEGA) * fs[1:7] + k1 * (ring(e[1:7], 2) + (e[:6] + e[2:])))
    e1[pl.ds(2, 6)] = e
    x = e[1:5]
    r = fs[2:6] + k1 * (ring(x, 2) + (e[:4] + e[2:])) - (c1[pl.ds(2, 4)] + (6.0 * k1 + both)) * x
    for q in range(quarter):
        t = r[2 * q] + r[2 * q + 1]
        rows[q, pl.ds(0, 32)] = pair(t, t, 2)
    f2 = [
        0.125 * (rows[q, pl.ds(0, 16, stride=2)] + rows[q, pl.ds(1, 16, stride=2)])
        for q in range(quarter)
    ]
    f2_out[...] = jnp.where(low, f2[0], f2[1])
    fourth = [
        to_dom(f2_out, f2_in.at[5 - k], wide_send, wide_recv, 6 + k, near[k]) for k in range(6)
    ]
    fifth = [
        to_dom(e1.at[pl.ds(4, 2)], e1.at[pl.ds(8, 2)], halo_send, halo_recv, 10, below),
        to_dom(e1.at[pl.ds(4, 2)], e1.at[pl.ds(0, 2)], halo_send, halo_recv, 11, above),
    ]
    for copy in fourth + fifth:
        copy.start()
    relay(1, 0)
    relay(1, 1)
    for copy in fourth:
        copy.wait_recv()

    f2s = []
    for k in range(3):
        f2s += split(f2_in[k], 2)
    f2s += f2
    for k in range(3, 6):
        f2s += split(f2_in[k], 2)
    f2v = jnp.stack(f2s[1:13])
    e = w2 * f2v
    for n in range(1, 4):
        inner = slice(n, 12 - n)
        x = e[1:-1]
        e = (1.0 - OMEGA) * x + w2[inner] * (f2v[inner] + k2 * (ring(x, 4) + (e[:-2] + e[2:])))

    for q in range(6):
        rows[q, pl.ds(0, 16, stride=2)] = e[q]
        rows[q, pl.ds(1, 16, stride=2)] = e[q]
    for copy in fifth:
        copy.wait_recv()
    e = jnp.stack([e1[l + 3] + rows[l // 2 + 2, pl.ds(0, 32)] for l in range(-3, 7)])
    for n in range(2):
        inner = slice(n, 8 - n)
        x = e[1:-1]
        e = (1.0 - OMEGA) * x + ws[inner] * (fs[inner] + k1 * (ring(x, 2) + (e[:-2] + e[2:])))
    for q in range(6):
        rows[q, pl.ds(0, 32, stride=2)] = e[q]
        rows[q, pl.ds(1, 32, stride=2)] = e[q]

    relay(2, 0)

    for copy in second:
        copy.wait_recv()

    def correct(q, carry):
        fields = split(rows[q], 1)
        for i in range(2):
            for h in range(2):
                ea[i, 2 * q + h] = eb[i, 2 * q + h] + fields[i]
        return carry

    lax.fori_loop(0, 6, correct, 0, unroll=2)
    for copy in second:
        copy.wait_send()

    def sweep_up(l, carry):
        for i in range(2):
            x = ea[i, l + 1]
            around = ring(x, 1) + (ea[i, l] + ea[i, l + 2])
            eb[i, l + 1] = (1.0 - OMEGA) * x + w[i, l] * (f[i, l] + KINETIC * around)
        return carry

    lax.fori_loop(0, layers + 2, sweep_up, 0, unroll=2)

    def sweep_last(l, carry):
        for i in range(2):
            x = eb[i, l + 2]
            around = ring(x, 1) + (eb[i, l + 1] + eb[i, l + 3])
            ea[i, l] = g[i, l + 1] + (
                (1.0 - OMEGA) * x + w[i, l + 1] * (f[i, l + 1] + KINETIC * around)
            )
        return carry

    lax.fori_loop(cut, layers, sweep_last, 0, unroll=2)

    @pl.when(is_outer)
    def _():
        visit.start()

    lax.fori_loop(0, cut, sweep_last, 0, unroll=2)

    def intersect(q, h, start, stop):
        def products(n, sums):
            l, r = lax.div(n, 8), pl.ds(pl.multiple_of(lax.rem(n, 8) * 8, 8), 8)
            u = [ea[i, l, r, :] for i in range(2)]
            new = []
            for c in range(2):
                x = orbs[2 * q + c, h, l, r, :]
                new += [sums[2 * c + i] + x * u[i] for i in range(2)]
            return tuple(new)

        sums = lax.fori_loop(start, stop, products, (jnp.zeros((8, 128), F32),) * 4, unroll=8)
        for m in range(4):
            row = pl.ds(4 * (m // 2) + 2 * h + m % 2, 1)
            found = jnp.sum(sums[m], axis=0, keepdims=True)
            gram[q, row, :] = found

    pair_side, odd = lax.div(chip, 2), lax.rem(chip, 2)
    ways = [
        (chip + 1 - 2 * odd, 1 - odd),
        (2 - pair_side, 1 - pair_side),
        (3 - 3 * pair_side, 1 - pair_side),
    ]
    for copy in own:
        copy.wait_recv()
    for h in range(2):
        intersect(chip, h, 0, 64)
    for n, (q, is_down) in enumerate(ways):
        away = (q - chip) * (2 * is_down - 1)
        slot_of = 12 + 6 * is_down + 2 * away
        block = 2 * q + 1 - core
        for h in range(2):
            if n == 1 and h == 1:
                relay(2, 1)
            if n < 2:
                hand(block, h, slot_of + h, mate).wait_recv()
                intersect(q, h, 0, 64)
                continue
            relay(3, h)

            @pl.when(is_outer)
            def _():
                hand(block, h, slot_of + h, mate, early).wait_recv()

            @pl.when(is_inner)
            def _():
                hand(block, h, slot_of + h, mate).wait_recv()
                intersect(q, h, 0, 64)

            @pl.when(is_outer)
            def _():
                intersect(q, h, 0, 8 * cut)

    @pl.when(is_inner)
    def _():
        visit.wait_recv()

        def products(n, sums):
            l, r = lax.div(n, 8), pl.ds(pl.multiple_of(lax.rem(n, 8) * 8, 8), 8)
            u = [guest[i, l, r, :] for i in range(2)]
            new = []
            for c in range(2):
                for h in range(2):
                    x = orbs[far - core + c, h, cut + l, r, :]
                    new += [sums[len(new) + i] + x * u[i] for i in range(2)]
            return tuple(new)

        sums = lax.fori_loop(0, 8 * LATE, products, (jnp.zeros((8, 128), F32),) * 8, unroll=4)
        for m in range(8):
            gram[4, pl.ds(m, 1), :] = jnp.sum(sums[m], axis=0, keepdims=True)
        answer.start()

    @pl.when(is_outer)
    def _():
        answer.wait_recv()
        last = 3 - 3 * lax.div(chip, 2)
        gram[last] = gram[last] + gram[5]

    diagonal = lax.broadcasted_iota(jnp.int32, (32, 128), 0) == lax.broadcasted_iota(
        jnp.int32, (32, 128), 1
    )

    def lay(column):
        return jnp.sum(jnp.where(diagonal, column, 0.0), axis=0, keepdims=True)

    part[0] = lay(jnp.sum(gram[pl.ds(0, 4)].reshape(32, 128), axis=1, keepdims=True))
    sixth = [
        to_dom(part.at[0], part.at[k], gram_send, gram_recv, k - 1, rest[k - 1])
        for k in range(1, doms)
    ]
    for copy in sixth:
        copy.start()

    @pl.when(chip == 2)
    def _():
        for copy in late_up:
            copy.start()

    @pl.when(chip == 1)
    def _():
        for copy in late_down:
            copy.start()

    for h in range(2):

        @pl.when(chip == 3)
        def _():
            hand(far, h, 26 + h, mate, late).wait_recv()
            late_share[h].start()

        @pl.when(chip == 0)
        def _():
            hand(far, h, 28 + h, mate, late).wait_recv()
            late_share[h].start()

    for copy in sixth:
        copy.wait_recv()
    total = jnp.sum(part[...], axis=0) * (1.0 / cells)
    coef[...] = jnp.broadcast_to(
        jnp.sum(jnp.where(diagonal, total, 0.0), axis=1, keepdims=True), (32, 128)
    )
    factors = [jnp.broadcast_to(coef[pl.ds(m, 1), :], (8, 128)) for m in range(32)]

    def project(n, carry):
        l, r = lax.div(n, 8), pl.ds(pl.multiple_of(lax.rem(n, 8) * 8, 8), 8)
        lost = [None, None]
        for j in range(16):
            x = orbs[j // 2, j % 2, l, r, :]
            for i in range(2):
                term = factors[2 * j + i] * x
                lost[i] = term if lost[i] is None else lost[i] + term
        for i in range(2):
            eb[i, l, r, :] = ea[i, l, r, :] - lost[i]
        return carry

    stores = []
    bounds = [0, 2, cut, layers - 1, layers]
    for k in range(4):
        if k == 2:

            @pl.when(is_outer)
            def _():
                for h in range(2):
                    hand(far + 1 - 2 * core, h, 30 + h, mate, late).wait_recv()

        lax.fori_loop(8 * bounds[k], 8 * bounds[k + 1], project, 0, unroll=2)
        part_of = pl.ds(bounds[k], bounds[k + 1] - bounds[k])
        stores.append(pltpu.make_async_copy(eb.at[:, part_of], out.at[:, part_of], load_sem.at[k]))
        stores[k].start()

    for copy in first + static + swap + third + fourth + fifth + sixth:
        copy.wait_send()
    for copy in own:
        copy.wait_send()
    for h in range(2):
        for n in range(3):

            @pl.when((chip >= n) & (chip < 3))
            def _():
                up(n, h).wait_send()

            @pl.when((chip <= 3 - n) & (chip > 0))
            def _():
                down(n, h).wait_send()

        for n in range(1, 4):

            @pl.when(chip >= n)
            def _():
                share_up(n, h).wait_send()

            @pl.when(chip <= 3 - n)
            def _():
                share_down(n, h).wait_send()

    @pl.when(is_outer)
    def _():
        for copy in late_share + [visit]:
            copy.wait_send()

    @pl.when(is_inner)
    def _():
        answer.wait_send()

    @pl.when(chip == 2)
    def _():
        for copy in late_up:
            copy.wait_send()

    @pl.when(chip == 1)
    def _():
        for copy in late_down:
            copy.wait_send()

    for store in stores:
        store.wait()


def on_device(orbitals, initial_guess, potential, perturbation, level_shifts, assignment):
    doms = lax.axis_size("dom")
    cells = orbitals.shape[1] * doms * orbitals.shape[2] * orbitals.shape[3]
    dma = pltpu.SemaphoreType.DMA
    vmem = pltpu.VMEM

    def field(*shape):
        return vmem(shape, F32)

    anywhere = pl.BlockSpec(memory_space=pltpu.HBM)
    return pl.pallas_call(
        functools.partial(kernel, cells),
        out_shape=jax.ShapeDtypeStruct(orbitals.shape, F32),
        in_specs=[anywhere] * 6,
        out_specs=anywhere,
        scratch_shapes=[
            field(8, 2, 8, 64, 128),
            field(2, 10, 64, 128),
            field(8, 64, 128),
            field(8, 64, 128),
            field(2, 2, 64, 128),
            field(2, 96, 128),
            field(2, 96, 128),
            field(16, 128),
            field(6, 16, 128),
            field(2, 2, 2, 64, 128),
            field(2, 2, 2, 64, 128),
            field(2, 10, 64, 128),
            field(2, 10, 64, 128),
            field(2, 12, 64, 128),
            field(2, 12, 64, 128),
            field(8, 32, 128),
            field(8, 32, 128),
            field(8, 32, 128),
            field(10, 32, 128),
            field(16, 128),
            field(6, 16, 128),
            field(6, 64, 128),
            field(6, 8, 128),
            field(2, LATE, 64, 128),
            field(doms, 1, 128),
            field(32, 128),
            pltpu.SMEM((16,), F32),
            pltpu.SMEM((2,), jnp.int32),
            dma((6,)),
            dma((12,)),
            dma((12,)),
            dma((12,)),
            dma((12,)),
            dma((34,)),
            dma((34,)),
            dma((doms - 1,)),
            dma((doms - 1,)),
        ],
        compiler_params=pltpu.CompilerParams(
            collective_id=0, has_side_effects=True, vmem_limit_bytes=67043328
        ),
        name="sternheimer",
    )(orbitals, initial_guess, potential, perturbation, level_shifts, assignment)


def solution(mesh):
    in_specs = (
        P("orb", "dom", None, None),
        P("orb", "dom", None, None),
        P("dom", None, None),
        P("dom", None, None),
        P(),
        P("orb"),
    )
    out_specs = P("orb", "dom", None, None)
    return jax.shard_map(
        on_device, mesh=mesh, in_specs=in_specs, out_specs=out_specs, check_vma=False
    )
```
